256 devices in a mesh: band: 128 (over x_lo, z, y, core), spin: 2 (over x_hi).
Axes of the slice: x: 4 (x_hi: 2, x_lo: 2; x = x_hi * 2 + x_lo), y: 4, z: 8, core: 2. Of those that a mesh axis runs over, the one named last changes fastest.
Arguments:
- coefficients: bfloat16 [2, 2, 256, 524288], P('spin', None, 'band'), may hold values from -1 to 1
- occupation: int32 [2, 256], P('spin', 'band'), may hold values from 0 to 1000
- miller: int32 [3, 524288], P(None, ('band', 'spin')), may hold values from -8 to 8
- density: float32 [2, 256, 128, 128], P('spin', 'band'), may hold values from 0.25 to 2
- local_factor: float32 [2, 256, 128, 128], P(None, None, 'band'), may hold values from -1.2 to 1.2
Outputs:
- stress: float32 [6], replicated
- kinetic_density: float32 [524288], P(('band', 'spin'))
- gradient_square: float32 [2, 256, 128, 128], P('spin', 'band')
The draws below stay inside these ranges and needn't reach their ends.
All inputs are finite; a program needn't handle non-finite values.
Results may differ from the reference program's by a relative error of at most 0.0003.
Values sent between devices are 32-bit elements; how exact they have to be, the bound alone decides.
A program may use at most 64 MiB of HBM per device.

```python
import math
import jax
import jax.numpy as jnp
from jax import lax

NPW = 524288
NX = 128
NY = 128
NZ = 256
BANDS = 256
SPINS = 2


def place_ends(result, stream_key, smallest, high):
    longest = result.shape.index(max(result.shape))
    spots = []
    for shift in (0, 1):
        where = [jax.random.randint(jax.random.fold_in(stream_key, axis), (), 0, length) for axis, length in enumerate(result.shape)]
        where[longest] = (where[longest] + shift) % result.shape[longest]
        spots.append(tuple(where))
    return result.at[spots[0]].set(smallest).at[spots[1]].set(high)


def with_spikes(values, rng, source, target, parts, factor):
    def block_of(dim):
        return (jnp.arange(values.shape[dim]) // (values.shape[dim] // parts)).reshape((-1,) + (1,) * (values.ndim - 1 - dim))

    one_side = jax.random.permutation(rng, parts)[block_of(target)]
    other_side = (block_of(target) + parts // 2) % parts
    return jnp.where((block_of(source) == one_side) | (block_of(source) == other_side), factor * values, values)


def steps_of(rng, dims, split, low, largest):
    def one(axis_at, blocks):
        draws = jax.random.uniform(jax.random.fold_in(jax.random.fold_in(rng, 6), axis_at), (blocks,), jnp.float32, low / len(split), largest / len(split))
        return jnp.repeat(jnp.exp(draws), dims[axis_at] // blocks).reshape((-1,) + (1,) * (len(dims) - axis_at - 1))

    level = one(*split[0])
    for cut in split[1:]:
        level = level * one(*cut)
    return level


def bell_draw(rng, dims, deviation, reach, split=(), kind=jnp.bfloat16):
    loudness = steps_of(rng, dims, split, -0.22, 0.18) if split else 1.0
    values = jax.random.normal(rng, dims, jnp.float32) * deviation * loudness
    return jnp.minimum(jnp.maximum(values, -reach), reach).astype(kind)


def heavy_noise(key, shape, width, limit, split, heavy, held_as=jnp.bfloat16):
    entries = width * jax.random.normal(key, shape, jnp.float32)
    if split:
        entries = entries * steps_of(key, shape, split, -0.22, 0.18)
    return jnp.clip(with_spikes(entries, jax.random.fold_in(key, 3), *heavy), -limit, limit).astype(held_as)


def setup_inputs(seed: int = 0) -> dict:
    keys = jax.random.split(jax.random.key(seed), 6)
    coefficients = heavy_noise(keys[0], (SPINS, 2, BANDS, NPW), (2 * BANDS) ** -0.5, 1.0, ((0, 2), (2, 128)), (2, 3, 128, 5.5))
    occupation = place_ends(jax.random.randint(keys[1], (SPINS, BANDS), 0, 1001), jax.random.fold_in(keys[1], 1), 0, 1000).astype(jnp.int32)
    miller = place_ends(jax.random.randint(keys[2], (3, NPW), -8, 9), jax.random.fold_in(keys[2], 1), -8, 8).astype(jnp.int32)
    density = jnp.clip(0.25 + 1.75 * jax.random.uniform(keys[3], (SPINS, NZ, NX, NY), jnp.float32) ** steps_of(keys[3], (SPINS, NZ, NX, NY), ((0, 2), (1, 128)), -0.2, 0.2), 0.25, 2.0)
    local_factor = bell_draw(keys[4], (2, NZ, NX, NY), 0.2, 1.2, ((2, 128),), jnp.float32)
    return {"coefficients": coefficients, "occupation": occupation, "miller": miller, "density": density, "local_factor": local_factor}


occupation_unit = 1000.0
kpoint = (0.25, 0.125, 0.375)
spacing = 0.25


def derivative_table(length):
    row_index = jnp.arange(length, dtype=jnp.int32)[:, None]
    col_index = jnp.arange(length, dtype=jnp.int32)[None, :]
    wrapped = jnp.mod(row_index - col_index, length)
    angles = (jnp.pi / length) * wrapped.astype(jnp.float32)
    on_diagonal = wrapped == 0
    sines = jnp.where(on_diagonal, 1.0, jnp.sin(angles))
    parity = 1.0 - 2.0 * jnp.mod(wrapped, 2).astype(jnp.float32)
    return jnp.where(on_diagonal, 0.0, 0.5 * parity * jnp.cos(angles) / sines).astype(jnp.float32)


def frequencies(length):
    positions = jnp.arange(length, dtype=jnp.int32)
    signed = jnp.where(positions >= length // 2, positions - length, positions)
    return (2.0 * jnp.pi / length) * signed.astype(jnp.float32)


def six_sums(weighting, first_axis, second_axis, third_axis):
    return jnp.stack([
        jnp.sum(weighting * first_axis * first_axis),
        jnp.sum(weighting * second_axis * second_axis),
        jnp.sum(weighting * third_axis * third_axis),
        jnp.sum(weighting * second_axis * third_axis),
        jnp.sum(weighting * first_axis * third_axis),
        jnp.sum(weighting * first_axis * second_axis)])


def reference(coefficients, occupation, miller, density, local_factor):
    highest = lax.Precision.HIGHEST
    weights = occupation.astype(jnp.float32) / occupation_unit
    band_block = math.gcd(BANDS, 32)

    def accumulate(counter, running):
        first_row = (jnp.asarray(counter).astype(jnp.int32) * band_block).astype(jnp.int32)
        piece = lax.dynamic_slice_in_dim(coefficients, first_row, band_block, 2).astype(jnp.float32)
        squares = piece[:, 0] * piece[:, 0] + piece[:, 1] * piece[:, 1]
        weight_piece = lax.dynamic_slice_in_dim(weights, first_row, band_block, 1)
        return running + jnp.einsum('sb,sbg->g', weight_piece, squares, precision=highest)

    kinetic_weight = lax.fori_loop(0, BANDS // band_block, accumulate, jnp.zeros((NPW,), jnp.float32))
    kvec = jnp.array(kpoint, jnp.float32)
    gvec = spacing * (miller.astype(jnp.float32) + kvec[:, None])
    kinetic_density = 0.5 * (gvec[0] ** 2 + gvec[1] ** 2 + gvec[2] ** 2) * kinetic_weight
    kinetic_stress = -six_sums(kinetic_weight, gvec[0], gvec[1], gvec[2]) / NPW

    deriv_x = derivative_table(NX)
    deriv_y = derivative_table(NY)
    deriv_z = derivative_table(NZ)
    grad_x = jnp.einsum('ik,szky->sziy', deriv_x, density, precision=highest)
    grad_y = jnp.einsum('ik,szxk->szxi', deriv_y, density, precision=highest)
    grad_z = jnp.einsum('ik,skxy->sixy', deriv_z, density, precision=highest)
    gradient_square = grad_x * grad_x + grad_y * grad_y + grad_z * grad_z
    kernel = density ** (-1.0 / 3.0) / (1.0 + gradient_square / (4.0 * density * density + 1.0))
    cell_count = NZ * NX * NY
    xc_stress = -six_sums(kernel, grad_x, grad_y, grad_z) / cell_count

    total_density = jnp.sum(density, axis=0)
    spectrum = jnp.fft.fftn(total_density) / cell_count
    real_part = jnp.real(spectrum)
    imag_part = jnp.imag(spectrum)
    freq_z = frequencies(NZ)[:, None, None]
    freq_x = frequencies(NX)[None, :, None]
    freq_y = frequencies(NY)[None, None, :]
    length_sq = freq_x * freq_x + freq_y * freq_y + freq_z * freq_z
    positive = length_sq > 0
    inverse = jnp.where(positive, 1.0 / jnp.where(positive, length_sq, 1.0), 0.0)
    hartree_weight = 4.0 * jnp.pi * (real_part * real_part + imag_part * imag_part) * inverse
    diagonal = jnp.array([1.0, 1.0, 1.0, 0.0, 0.0, 0.0], jnp.float32)
    hartree_stress = 2.0 * six_sums(hartree_weight * inverse, freq_x, freq_y, freq_z) - diagonal * jnp.sum(hartree_weight)
    local_weight = 2.0 * (real_part * local_factor[0] + imag_part * local_factor[1])
    local_stress = six_sums(local_weight, freq_x, freq_y, freq_z)
    stress = kinetic_stress + hartree_stress + local_stress + xc_stress
    return stress, kinetic_density, gradient_square
```

```python
import jax
import jax.numpy as jnp
from jax import lax
from jax.experimental import pallas as pl
from jax.experimental.pallas import tpu as pltpu
from jax.sharding import Mesh
from jax.sharding import PartitionSpec as P

NPW = 524288
NX = 128
NY = 128
NZ = 256
BAND_SPIN = ("band_0", "band_1", "band_2", "band_3", "spin")
BAND = ("band_0", "band_1", "band_2", "band_3")


occupation_unit = 1000.0
kpoint = (0.25, 0.125, 0.375)
spacing = 0.25


def sent_together(arrays, axis, split_dim, concat_dim, along):
    both = jnp.concatenate(arrays, axis=along)
    result, at, gathered = (
        lax.all_to_all(both, axis, split_axis=split_dim, concat_axis=concat_dim, tiled=True),
        0,
        [],
    )
    for a in arrays:
        gathered.append(lax.slice_in_dim(result, at, at + a.shape[along], axis=along))
        at += a.shape[along]
    return tuple(gathered)


def sent_to_all(shard, axis):
    length = lax.axis_size(axis)
    return lax.all_to_all(
        jnp.broadcast_to(shard[None], (length, *shard.shape)), axis, 0, 0, tiled=True
    )


def over_copies(shard, axis):
    return sent_to_all(shard, axis).sum(axis=0)


def packed_total(arrays, axis):
    flat, at, gathered = (jnp.concatenate([a.reshape(-1) for a in arrays]), 0, [])
    subtotal = over_copies(flat, axis)
    for a in arrays:
        gathered.append(subtotal[at : at + a.size].reshape(a.shape))
        at += a.size
    return tuple(gathered)


def derivative_table(length):
    row_index = jnp.arange(length, dtype=jnp.int32)[:, None]
    col_index = jnp.arange(length, dtype=jnp.int32)[None, :]
    wrapped = jnp.mod(row_index - col_index, length)
    angles = jnp.pi / length * wrapped.astype(jnp.float32)
    on_diagonal = wrapped == 0
    sines = jnp.where(on_diagonal, 1.0, jnp.sin(angles))
    parity = 1.0 - 2.0 * jnp.mod(wrapped, 2).astype(jnp.float32)
    return jnp.where(on_diagonal, 0.0, 0.5 * parity * jnp.cos(angles) / sines)


def fourier_tables(length):
    positions = jnp.arange(length, dtype=jnp.int32)
    phases = jnp.mod(positions[:, None] * positions[None, :], length).astype(jnp.float32) * (
        2.0 * jnp.pi / length
    )
    return (jnp.cos(phases), jnp.sin(phases))


def frequencies(length):
    positions = jnp.arange(length, dtype=jnp.int32)
    signed = jnp.where(positions >= length // 2, positions - length, positions)
    return 2.0 * jnp.pi / length * signed.astype(jnp.float32)


def six_sums(weighting, first_axis, second_axis, third_axis):
    return jnp.stack(
        [
            jnp.sum(weighting * first_axis * first_axis),
            jnp.sum(weighting * second_axis * second_axis),
            jnp.sum(weighting * third_axis * third_axis),
            jnp.sum(weighting * second_axis * third_axis),
            jnp.sum(weighting * first_axis * third_axis),
            jnp.sum(weighting * first_axis * second_axis),
        ]
    )


def xc_terms(dens_part, grad_x, grad_y, grad_z, cell_count):
    square = grad_x * grad_x + grad_y * grad_y + grad_z * grad_z
    kernel = dens_part ** (-1.0 / 3.0) / (1.0 + square / (4.0 * dens_part * dens_part + 1.0))
    return (square, -six_sums(kernel, grad_x, grad_y, grad_z) / cell_count)


AXIS_X, AXIS_XLO, AXIS_Z, AXIS_Y, AXIS_C = "spin", "band_0", "band_1", "band_2", "band_3"
MESH = pl.DeviceIdType.MESH


def place():
    x = lax.axis_index(AXIS_X) * 2 + lax.axis_index(AXIS_XLO)
    return x, lax.axis_index(AXIS_Z), lax.axis_index(AXIS_Y), lax.axis_index(AXIS_C)


def at_x(x):
    return {AXIS_X: x // 2, AXIS_XLO: x % 2}


def greet(groups):
    barrier = pltpu.get_barrier_semaphore()
    for peer in groups:
        pl.semaphore_signal(barrier, inc=1, device_id=peer, device_id_type=MESH)
    pl.semaphore_wait(barrier, len(groups))


def kinetic_kernel(occ, coef, miller, density, tile, part, twin, qa, qb, ra, rb, a1, b1, ra2, rb2, ab, rz, tmp, ssem, rsem):
    x, z, y, c = place()
    other = 1 - c
    x_peers = [lax.rem(x + d, 4) for d in (1, 2, 3)]
    y_peers = [lax.rem(y + d, 4) for d in (1, 2, 3)]
    z_peers = [lax.rem(z + d, 8) for d in range(1, 8)]
    greet(
        [{AXIS_C: other}]
        + [at_x(p) for p in x_peers]
        + [{AXIS_Y: p} for p in y_peers]
        + [{AXIS_Z: p} for p in z_peers]
    )
    pending = []

    def send(src, dst, k, peer):
        copy = pltpu.make_async_remote_copy(
            src_ref=src, dst_ref=dst, send_sem=ssem.at[k], recv_sem=rsem.at[k], device_id=peer, device_id_type=MESH
        )
        copy.start()
        pending.append(copy)
        return copy

    w0 = jnp.full((64, 128), occ[0, 0].astype(jnp.float32)) / occupation_unit
    w1 = jnp.full((64, 128), occ[0, 1].astype(jnp.float32)) / occupation_unit
    twins = []
    for q in range(4):

        def squares(i, carry):
            rows = pl.ds(pl.multiple_of(i * 128, 128), 128)
            re = coef[0, rows, :].astype(jnp.float32)
            im = coef[1, rows, :].astype(jnp.float32)
            tmp[...] = re * re + im * im
            both = w0 * tmp[pl.ds(0, 64, stride=2), :] + w1 * tmp[pl.ds(1, 64, stride=2), :]
            part[i] = both.reshape(2, 32, 128)
            return carry

        lax.fori_loop(q * 16, q * 16 + 16, squares, 0)
        twins.append(send(part.at[pl.ds(q * 16, 16), other], twin.at[pl.ds(q * 16, 16)], q, {AXIS_C: other}))
    for q in range(4):
        twins[q].wait_recv()

        def add_twin(i, carry):
            x_lo, zz, yy = i // 32, lax.rem(i // 4, 8), lax.rem(i, 4)
            v = part[i, c] + twin[i]
            for x_hi in range(2):
                pos = x_hi * 2 + x_lo
                qa[pos, yy * 8 + zz] = v[x_hi * 16 : x_hi * 16 + 8]
                qb[yy, pos * 8 + zz] = v[x_hi * 16 + 8 : x_hi * 16 + 16]
            return carry

        lax.fori_loop(q * 16, q * 16 + 16, add_twin, 0)
    first_a = [send(qa.at[p], ra.at[d], 4 + d, at_x(p)) for d, p in enumerate(x_peers)]
    first_b = [send(qb.at[p], rb.at[d], 7 + d, {AXIS_Y: p}) for d, p in enumerate(y_peers)]
    for copy in first_a:
        copy.wait_recv()
    for t in range(4):
        sub = pl.ds(t * 8, 8)
        a1[t] = (qa[x, sub] + ra[0, sub]) + (ra[1, sub] + ra[2, sub])
    second_a = [send(a1.at[p], ra2.at[d], 10 + d, {AXIS_Y: p}) for d, p in enumerate(y_peers)]
    for copy in first_b:
        copy.wait_recv()
    for t in range(4):
        sub = pl.ds(t * 8, 8)
        b1[t] = (qb[y, sub] + rb[0, sub]) + (rb[1, sub] + rb[2, sub])
    second_b = [send(b1.at[p], rb2.at[d], 13 + d, at_x(p)) for d, p in enumerate(x_peers)]
    for copy in second_a:
        copy.wait_recv()
    ab[:, 0] = (a1[y] + ra2[0]) + (ra2[1] + ra2[2])
    for copy in second_b:
        copy.wait_recv()
    ab[:, 1] = (b1[x] + rb2[0]) + (rb2[1] + rb2[2])
    last = [send(ab.at[p], rz.at[d], 16 + d, {AXIS_Z: p}) for d, p in enumerate(z_peers)]
    g = [spacing * (miller[a].astype(jnp.float32) + kpoint[a]) for a in range(3)]
    for copy in last:
        copy.wait_recv()
    weight = ab[z]
    for d in range(7):
        weight = weight + rz[d]
    weight = weight.reshape(16, 128)
    density[...] = 0.5 * (g[0] * g[0] + g[1] * g[1] + g[2] * g[2]) * weight
    scaled = weight * (-1.0 / NPW)
    rows = [
        jnp.sum(scaled * g[a] * g[b], axis=0, keepdims=True)
        for a, b in ((0, 0), (1, 1), (2, 2), (1, 2), (0, 2), (0, 1))
    ]
    tile[...] = jnp.concatenate(rows + [jnp.zeros((2, 128), jnp.float32)], axis=0)
    for copy in pending:
        copy.wait_send()


def kinetic(coefficients, occupation, miller):
    pairs = coefficients[0].reshape(2, 2, NPW // 128, 128).transpose(0, 2, 1, 3).reshape(2, NPW // 64, 128)
    f32 = jnp.float32
    vmem = pl.BlockSpec(memory_space=pltpu.VMEM)
    return pl.pallas_call(
        kinetic_kernel,
        out_shape=(jax.ShapeDtypeStruct((16, 128), f32), jax.ShapeDtypeStruct((8, 128), f32)),
        in_specs=[pl.BlockSpec(memory_space=pltpu.SMEM), vmem, vmem],
        out_specs=(vmem, vmem),
        scratch_shapes=[
            pltpu.VMEM((64, 2, 32, 128), f32),
            pltpu.VMEM((64, 32, 128), f32),
            pltpu.VMEM((4, 32, 8, 128), f32),
            pltpu.VMEM((4, 32, 8, 128), f32),
            pltpu.VMEM((3, 32, 8, 128), f32),
            pltpu.VMEM((3, 32, 8, 128), f32),
            pltpu.VMEM((4, 8, 8, 128), f32),
            pltpu.VMEM((4, 8, 8, 128), f32),
            pltpu.VMEM((3, 8, 8, 128), f32),
            pltpu.VMEM((3, 8, 8, 128), f32),
            pltpu.VMEM((8, 2, 8, 128), f32),
            pltpu.VMEM((7, 2, 8, 128), f32),
            pltpu.VMEM((128, 128), f32),
            pltpu.SemaphoreType.DMA((23,)),
            pltpu.SemaphoreType.DMA((23,)),
        ],
        compiler_params=pltpu.CompilerParams(collective_id=0, has_side_effects=True),
    )(occupation, pairs, miller.reshape(3, 16, 128))


def total_kernel(tile, out, rz, ry, rx, held, ssem, rsem):
    x, z, y, c = place()
    stages = (
        (rz, z, [(lax.rem(z + d, 8), {AXIS_Z: lax.rem(z + d, 8)}) for d in range(1, 8)], 8),
        (ry, y, [(lax.rem(y + d, 4), {AXIS_Y: lax.rem(y + d, 4)}) for d in range(1, 4)], 4),
        (rx, x * 2 + c, [
            (None, {**at_x(lax.rem(x + d // 2, 4)), AXIS_C: lax.rem(c + d % 2, 2)}) for d in range(1, 8)
        ], 8),
    )
    greet([peer for stage in stages for _, peer in stage[2]])
    pending, k = [], 0
    held[0] = tile[...]
    for at, (slots, me, peers, count) in enumerate(stages):
        copies = []
        for _, peer in peers:
            copy = pltpu.make_async_remote_copy(
                src_ref=held.at[at], dst_ref=slots.at[me], send_sem=ssem.at[k], recv_sem=rsem.at[k],
                device_id=peer, device_id_type=MESH,
            )
            copy.start()
            copies.append(copy)
            k += 1
        slots[me] = held[at]
        for copy in copies:
            copy.wait_recv()
        pending += copies
        subtotal = slots[0]
        for j in range(1, count):
            subtotal = subtotal + slots[j]
        held[at + 1] = subtotal
    for a in range(6):
        out[a] = jnp.sum(subtotal[a : a + 1, :])
    for copy in pending:
        copy.wait_send()


def total(tile):
    f32 = jnp.float32
    return pl.pallas_call(
        total_kernel,
        out_shape=jax.ShapeDtypeStruct((6,), f32),
        in_specs=[pl.BlockSpec(memory_space=pltpu.VMEM)],
        out_specs=pl.BlockSpec(memory_space=pltpu.SMEM),
        scratch_shapes=[
            pltpu.VMEM((8, 8, 128), f32),
            pltpu.VMEM((4, 8, 128), f32),
            pltpu.VMEM((8, 8, 128), f32),
            pltpu.VMEM((4, 8, 128), f32),
            pltpu.SemaphoreType.DMA((17,)),
            pltpu.SemaphoreType.DMA((17,)),
        ],
        compiler_params=pltpu.CompilerParams(collective_id=1, has_side_effects=True),
    )(tile)


def shards(coefficients, occupation, miller, density, local_factor):
    highest = lax.Precision.HIGHEST
    kinetic_density, tile = kinetic(coefficients, occupation, miller)
    band_devices = lax.axis_size(BAND)
    cell_count = density.shape[1] * band_devices * density.shape[2] * density.shape[3]
    deriv_x = derivative_table(NX)
    deriv_y = derivative_table(NY)
    deriv_z = derivative_table(NZ)
    cosine_x, sine_x = fourier_tables(NX)
    cosine_y, sine_y = fourier_tables(NY)
    cosine_z, sine_z = fourier_tables(NZ)
    grad_x = jnp.einsum("ik,szky->sziy", deriv_x, density, precision=highest)
    grad_y = jnp.einsum("ik,szxk->szxi", deriv_y, density, precision=highest)
    along_real = jnp.einsum("mj,szxj->szxm", cosine_y, density, precision=highest)
    along_imag = -jnp.einsum("mj,szxj->szxm", sine_y, density, precision=highest)
    plane_real = jnp.einsum("mj,szjy->szmy", cosine_x, along_real, precision=highest) + jnp.einsum(
        "mj,szjy->szmy", sine_x, along_imag, precision=highest
    )
    plane_imag = jnp.einsum("mj,szjy->szmy", cosine_x, along_imag, precision=highest) - jnp.einsum(
        "mj,szjy->szmy", sine_x, along_real, precision=highest
    )
    dens_col, real_col, imag_col = sent_together((density, plane_real, plane_imag), BAND, 2, 1, 0)
    gradz_col = jnp.einsum("ik,skxy->sixy", deriv_z, dens_col, precision=highest)
    grad_z = lax.all_to_all(gradz_col, BAND, split_axis=1, concat_axis=2, tiled=True)
    gradient_square, xc_stress = xc_terms(density, grad_x, grad_y, grad_z, cell_count)
    spec_real = (
        jnp.einsum("mj,jxy->mxy", cosine_z, real_col[0], precision=highest)
        + jnp.einsum("mj,jxy->mxy", sine_z, imag_col[0], precision=highest)
    ) / cell_count
    spec_imag = (
        jnp.einsum("mj,jxy->mxy", cosine_z, imag_col[0], precision=highest)
        - jnp.einsum("mj,jxy->mxy", sine_z, real_col[0], precision=highest)
    ) / cell_count
    total_real, total_imag = packed_total((spec_real, spec_imag), "spin")
    local_rows = real_col.shape[2]
    first_column = lax.axis_index(BAND) * local_rows
    freq_z = frequencies(NZ)[:, None, None]
    freq_x = lax.dynamic_slice_in_dim(frequencies(NX), first_column, local_rows, 0)[None, :, None]
    freq_y = frequencies(NY)[None, None, :]
    length_sq = freq_x * freq_x + freq_y * freq_y + freq_z * freq_z
    positive = length_sq > 0
    inverse = jnp.where(positive, 1.0 / jnp.where(positive, length_sq, 1.0), 0.0)
    hartree_weight = 4.0 * jnp.pi * (total_real * total_real + total_imag * total_imag) * inverse
    diagonal = jnp.array([1.0, 1.0, 1.0, 0.0, 0.0, 0.0], jnp.float32)
    hartree_stress = 2.0 * six_sums(
        hartree_weight * inverse, freq_x, freq_y, freq_z
    ) - diagonal * jnp.sum(hartree_weight)
    local_weight = 2.0 * (total_real * local_factor[0] + total_imag * local_factor[1])
    local_stress = six_sums(local_weight, freq_x, freq_y, freq_z)
    spin_share = 1.0 / lax.axis_size("spin")
    partial_stress = spin_share * (hartree_stress + local_stress) + xc_stress
    stress = total(tile + jnp.pad(partial_stress[:, None], ((0, 2), (0, 127))))
    return (stress, kinetic_density.reshape(-1), gradient_square)


def solution(mesh):
    finer = Mesh(
        mesh.devices.reshape(2, 8, 4, 2, mesh.shape["spin"]),
        ("band_0", "band_1", "band_2", "band_3", "spin"),
    )
    return jax.shard_map(
        shards,
        mesh=finer,
        in_specs=(
            P("spin", None, BAND, None),
            P("spin", BAND),
            P(None, BAND_SPIN),
            P("spin", BAND, None, None),
            P(None, None, BAND, None),
        ),
        out_specs=(P(), P(BAND_SPIN), P("spin", BAND, None, None)),
        check_vma=False,
    )
```

```python
import functools

import jax
import jax.numpy as jnp
from jax import lax
from jax.experimental import pallas as pl
from jax.experimental.pallas import tpu as pltpu
from jax.sharding import Mesh
from jax.sharding import PartitionSpec as P

NPW = 524288
NX = 128
NY = 128
NZ = 256
BAND_SPIN = ("band_0", "band_1", "band_2", "band_3", "spin")
BAND = ("band_0", "band_1", "band_2", "band_3")


occupation_unit = 1000.0
kpoint = (0.25, 0.125, 0.375)
spacing = 0.25


def sent_to_all(shard, axis):
    length = lax.axis_size(axis)
    return lax.all_to_all(
        jnp.broadcast_to(shard[None], (length, *shard.shape)), axis, 0, 0, tiled=True
    )


def over_copies(shard, axis):
    return sent_to_all(shard, axis).sum(axis=0)


def packed_total(arrays, axis):
    flat, at, gathered = (jnp.concatenate([a.reshape(-1) for a in arrays]), 0, [])
    subtotal = over_copies(flat, axis)
    for a in arrays:
        gathered.append(subtotal[at : at + a.size].reshape(a.shape))
        at += a.size
    return tuple(gathered)


def derivative_table(length):
    row_index = jnp.arange(length, dtype=jnp.int32)[:, None]
    col_index = jnp.arange(length, dtype=jnp.int32)[None, :]
    wrapped = jnp.mod(row_index - col_index, length)
    angles = jnp.pi / length * wrapped.astype(jnp.float32)
    on_diagonal = wrapped == 0
    sines = jnp.where(on_diagonal, 1.0, jnp.sin(angles))
    parity = 1.0 - 2.0 * jnp.mod(wrapped, 2).astype(jnp.float32)
    return jnp.where(on_diagonal, 0.0, 0.5 * parity * jnp.cos(angles) / sines)


def fourier_tables(length):
    positions = jnp.arange(length, dtype=jnp.int32)
    phases = jnp.mod(positions[:, None] * positions[None, :], length).astype(jnp.float32) * (
        2.0 * jnp.pi / length
    )
    return (jnp.cos(phases), jnp.sin(phases))


def frequencies(length):
    positions = jnp.arange(length, dtype=jnp.int32)
    signed = jnp.where(positions >= length // 2, positions - length, positions)
    return 2.0 * jnp.pi / length * signed.astype(jnp.float32)


def six_sums(weighting, first_axis, second_axis, third_axis):
    return jnp.stack(
        [
            jnp.sum(weighting * first_axis * first_axis),
            jnp.sum(weighting * second_axis * second_axis),
            jnp.sum(weighting * third_axis * third_axis),
            jnp.sum(weighting * second_axis * third_axis),
            jnp.sum(weighting * first_axis * third_axis),
            jnp.sum(weighting * first_axis * second_axis),
        ]
    )


def xc_terms(dens_part, grad_x, grad_y, grad_z, cell_count):
    square = grad_x * grad_x + grad_y * grad_y + grad_z * grad_z
    kernel = dens_part ** (-1.0 / 3.0) / (1.0 + square / (4.0 * dens_part * dens_part + 1.0))
    return (square, -six_sums(kernel, grad_x, grad_y, grad_z) / cell_count)


AXIS_X, AXIS_XLO, AXIS_Z, AXIS_Y, AXIS_C = "spin", "band_0", "band_1", "band_2", "band_3"
MESH = pl.DeviceIdType.MESH


def place():
    x = lax.axis_index(AXIS_X) * 2 + lax.axis_index(AXIS_XLO)
    return x, lax.axis_index(AXIS_Z), lax.axis_index(AXIS_Y), lax.axis_index(AXIS_C)


def at_x(x):
    return {AXIS_X: x // 2, AXIS_XLO: x % 2}


def greet(groups):
    barrier = pltpu.get_barrier_semaphore()
    for peer in groups:
        pl.semaphore_signal(barrier, inc=1, device_id=peer, device_id_type=MESH)
    pl.semaphore_wait(barrier, len(groups))


def kinetic_kernel(occ, coef, miller, density, tile, part, twin, qa, qb, ra, rb, a1, b1, ra2, rb2, ab, rz, tmp, ssem, rsem):
    x, z, y, c = place()
    other = 1 - c
    x_peers = [lax.rem(x + d, 4) for d in (1, 2, 3)]
    y_peers = [lax.rem(y + d, 4) for d in (1, 2, 3)]
    z_peers = [lax.rem(z + d, 8) for d in range(1, 8)]
    greet(
        [{AXIS_C: other}]
        + [at_x(p) for p in x_peers]
        + [{AXIS_Y: p} for p in y_peers]
        + [{AXIS_Z: p} for p in z_peers]
    )
    pending = []

    def send(src, dst, k, peer):
        copy = pltpu.make_async_remote_copy(
            src_ref=src, dst_ref=dst, send_sem=ssem.at[k], recv_sem=rsem.at[k], device_id=peer, device_id_type=MESH
        )
        copy.start()
        pending.append(copy)
        return copy

    w0 = jnp.full((64, 128), occ[0, 0].astype(jnp.float32)) / occupation_unit
    w1 = jnp.full((64, 128), occ[0, 1].astype(jnp.float32)) / occupation_unit
    twins = []
    for q in range(4):

        def squares(i, carry):
            rows = pl.ds(pl.multiple_of(i * 128, 128), 128)
            re = coef[0, rows, :].astype(jnp.float32)
            im = coef[1, rows, :].astype(jnp.float32)
            tmp[...] = re * re + im * im
            both = w0 * tmp[pl.ds(0, 64, stride=2), :] + w1 * tmp[pl.ds(1, 64, stride=2), :]
            part[i] = both.reshape(2, 32, 128)
            return carry

        lax.fori_loop(q * 16, q * 16 + 16, squares, 0)
        twins.append(send(part.at[pl.ds(q * 16, 16), other], twin.at[pl.ds(q * 16, 16)], q, {AXIS_C: other}))
    for q in range(4):
        twins[q].wait_recv()

        def add_twin(i, carry):
            x_lo, zz, yy = i // 32, lax.rem(i // 4, 8), lax.rem(i, 4)
            v = part[i, c] + twin[i]
            for x_hi in range(2):
                pos = x_hi * 2 + x_lo
                qa[pos, yy * 8 + zz] = v[x_hi * 16 : x_hi * 16 + 8]
                qb[yy, pos * 8 + zz] = v[x_hi * 16 + 8 : x_hi * 16 + 16]
            return carry

        lax.fori_loop(q * 16, q * 16 + 16, add_twin, 0)
    first_a = [send(qa.at[p], ra.at[d], 4 + d, at_x(p)) for d, p in enumerate(x_peers)]
    first_b = [send(qb.at[p], rb.at[d], 7 + d, {AXIS_Y: p}) for d, p in enumerate(y_peers)]
    for copy in first_a:
        copy.wait_recv()
    for t in range(4):
        sub = pl.ds(t * 8, 8)
        a1[t] = (qa[x, sub] + ra[0, sub]) + (ra[1, sub] + ra[2, sub])
    second_a = [send(a1.at[p], ra2.at[d], 10 + d, {AXIS_Y: p}) for d, p in enumerate(y_peers)]
    for copy in first_b:
        copy.wait_recv()
    for t in range(4):
        sub = pl.ds(t * 8, 8)
        b1[t] = (qb[y, sub] + rb[0, sub]) + (rb[1, sub] + rb[2, sub])
    second_b = [send(b1.at[p], rb2.at[d], 13 + d, at_x(p)) for d, p in enumerate(x_peers)]
    for copy in second_a:
        copy.wait_recv()
    ab[:, 0] = (a1[y] + ra2[0]) + (ra2[1] + ra2[2])
    for copy in second_b:
        copy.wait_recv()
    ab[:, 1] = (b1[x] + rb2[0]) + (rb2[1] + rb2[2])
    last = [send(ab.at[p], rz.at[d], 16 + d, {AXIS_Z: p}) for d, p in enumerate(z_peers)]
    g = [spacing * (miller[a].astype(jnp.float32) + kpoint[a]) for a in range(3)]
    for copy in last:
        copy.wait_recv()
    weight = ab[z]
    for d in range(7):
        weight = weight + rz[d]
    weight = weight.reshape(16, 128)
    density[...] = 0.5 * (g[0] * g[0] + g[1] * g[1] + g[2] * g[2]) * weight
    scaled = weight * (-1.0 / NPW)
    rows = [
        jnp.sum(scaled * g[a] * g[b], axis=0, keepdims=True)
        for a, b in ((0, 0), (1, 1), (2, 2), (1, 2), (0, 2), (0, 1))
    ]
    tile[...] = jnp.concatenate(rows + [jnp.zeros((2, 128), jnp.float32)], axis=0)
    for copy in pending:
        copy.wait_send()


def kinetic(coefficients, occupation, miller):
    pairs = coefficients[0].reshape(2, 2, NPW // 128, 128).transpose(0, 2, 1, 3).reshape(2, NPW // 64, 128)
    f32 = jnp.float32
    vmem = pl.BlockSpec(memory_space=pltpu.VMEM)
    return pl.pallas_call(
        kinetic_kernel,
        out_shape=(jax.ShapeDtypeStruct((16, 128), f32), jax.ShapeDtypeStruct((8, 128), f32)),
        in_specs=[pl.BlockSpec(memory_space=pltpu.SMEM), vmem, vmem],
        out_specs=(vmem, vmem),
        scratch_shapes=[
            pltpu.VMEM((64, 2, 32, 128), f32),
            pltpu.VMEM((64, 32, 128), f32),
            pltpu.VMEM((4, 32, 8, 128), f32),
            pltpu.VMEM((4, 32, 8, 128), f32),
            pltpu.VMEM((3, 32, 8, 128), f32),
            pltpu.VMEM((3, 32, 8, 128), f32),
            pltpu.VMEM((4, 8, 8, 128), f32),
            pltpu.VMEM((4, 8, 8, 128), f32),
            pltpu.VMEM((3, 8, 8, 128), f32),
            pltpu.VMEM((3, 8, 8, 128), f32),
            pltpu.VMEM((8, 2, 8, 128), f32),
            pltpu.VMEM((7, 2, 8, 128), f32),
            pltpu.VMEM((128, 128), f32),
            pltpu.SemaphoreType.DMA((23,)),
            pltpu.SemaphoreType.DMA((23,)),
        ],
        compiler_params=pltpu.CompilerParams(collective_id=0, has_side_effects=True),
    )(occupation, pairs, miller.reshape(3, 16, 128))


def total_kernel(tile, out, rz, ry, rx, held, ssem, rsem):
    x, z, y, c = place()
    stages = (
        (rz, z, [(lax.rem(z + d, 8), {AXIS_Z: lax.rem(z + d, 8)}) for d in range(1, 8)], 8),
        (ry, y, [(lax.rem(y + d, 4), {AXIS_Y: lax.rem(y + d, 4)}) for d in range(1, 4)], 4),
        (rx, x * 2 + c, [
            (None, {**at_x(lax.rem(x + d // 2, 4)), AXIS_C: lax.rem(c + d % 2, 2)}) for d in range(1, 8)
        ], 8),
    )
    greet([peer for stage in stages for _, peer in stage[2]])
    pending, k = [], 0
    held[0] = tile[...]
    for at, (slots, me, peers, count) in enumerate(stages):
        copies = []
        for _, peer in peers:
            copy = pltpu.make_async_remote_copy(
                src_ref=held.at[at], dst_ref=slots.at[me], send_sem=ssem.at[k], recv_sem=rsem.at[k],
                device_id=peer, device_id_type=MESH,
            )
            copy.start()
            copies.append(copy)
            k += 1
        slots[me] = held[at]
        for copy in copies:
            copy.wait_recv()
        pending += copies
        subtotal = slots[0]
        for j in range(1, count):
            subtotal = subtotal + slots[j]
        held[at + 1] = subtotal
    for a in range(6):
        out[a] = jnp.sum(subtotal[a : a + 1, :])
    for copy in pending:
        copy.wait_send()


def total(tile):
    f32 = jnp.float32
    return pl.pallas_call(
        total_kernel,
        out_shape=jax.ShapeDtypeStruct((6,), f32),
        in_specs=[pl.BlockSpec(memory_space=pltpu.VMEM)],
        out_specs=pl.BlockSpec(memory_space=pltpu.SMEM),
        scratch_shapes=[
            pltpu.VMEM((8, 8, 128), f32),
            pltpu.VMEM((4, 8, 128), f32),
            pltpu.VMEM((8, 8, 128), f32),
            pltpu.VMEM((4, 8, 128), f32),
            pltpu.SemaphoreType.DMA((17,)),
            pltpu.SemaphoreType.DMA((17,)),
        ],
        compiler_params=pltpu.CompilerParams(collective_id=1, has_side_effects=True),
    )(tile)


def exchange_kernel(count, *refs):
    outgoing, incoming = refs[:count], refs[count : 2 * count]
    far, ssem, rsem = refs[2 * count :]
    x, z, y, c = place()
    x_lo = lax.rem(x, 2)
    me = ((x_lo * 8 + z) * 4 + y) * 2 + c
    z_peers = [{AXIS_Z: lax.rem(z + d, 8)} for d in range(1, 8)]
    plane = [
        {AXIS_XLO: lax.rem(x_lo + d // 8, 2), AXIS_Y: lax.rem(y + d // 2, 4), AXIS_C: lax.rem(c + d, 2)}
        for d in range(1, 16)
    ]
    greet(z_peers + plane)
    for peer in z_peers:
        pl.semaphore_signal(far, inc=1, device_id=peer, device_id_type=MESH)
    pl.semaphore_wait(far, 7)

    def push(d, carry):
        t = lax.rem(me + d, 128)
        peer = {AXIS_XLO: t // 64, AXIS_Z: lax.rem(t // 8, 8), AXIS_Y: lax.rem(t // 2, 4), AXIS_C: lax.rem(t, 2)}
        for k in range(count):
            pltpu.make_async_remote_copy(
                src_ref=outgoing[k].at[t], dst_ref=incoming[k].at[me], send_sem=ssem.at[k], recv_sem=rsem.at[k],
                device_id=peer, device_id_type=MESH,
            ).start()
        return carry

    lax.fori_loop(1, 128, push, 0)
    for k in range(count):
        incoming[k][me] = outgoing[k][me]
    for k in range(count):
        bulk = incoming[k].at[pl.ds(0, 127)]
        pltpu.make_async_copy(bulk, bulk, rsem.at[k]).wait()
        pltpu.make_async_copy(bulk, bulk, ssem.at[k]).wait()


def exchange(arrays, collective_id):
    count = len(arrays)
    vmem = pl.BlockSpec(memory_space=pltpu.VMEM)
    return pl.pallas_call(
        functools.partial(exchange_kernel, count),
        out_shape=tuple(jax.ShapeDtypeStruct((128, 2, 128), jnp.float32) for _ in arrays),
        in_specs=[vmem] * count,
        out_specs=(vmem,) * count,
        scratch_shapes=[
            pltpu.SemaphoreType.REGULAR,
            pltpu.SemaphoreType.DMA((count,)),
            pltpu.SemaphoreType.DMA((count,)),
        ],
        compiler_params=pltpu.CompilerParams(collective_id=collective_id, has_side_effects=True),
    )(*arrays)


def to_columns(arrays, collective_id):
    gathered = exchange([a[0].transpose(1, 0, 2) for a in arrays], collective_id)
    return tuple(g.reshape(1, NZ, 1, NY) for g in gathered)


def shards(coefficients, occupation, miller, density, local_factor):
    highest = lax.Precision.HIGHEST
    kinetic_density, tile = kinetic(coefficients, occupation, miller)
    band_devices = lax.axis_size(BAND)
    cell_count = density.shape[1] * band_devices * density.shape[2] * density.shape[3]
    deriv_x = derivative_table(NX)
    deriv_y = derivative_table(NY)
    deriv_z = derivative_table(NZ)
    cosine_x, sine_x = fourier_tables(NX)
    cosine_y, sine_y = fourier_tables(NY)
    cosine_z, sine_z = fourier_tables(NZ)
    grad_x = jnp.einsum("ik,szky->sziy", deriv_x, density, precision=highest)
    grad_y = jnp.einsum("ik,szxk->szxi", deriv_y, density, precision=highest)
    along_real = jnp.einsum("mj,szxj->szxm", cosine_y, density, precision=highest)
    along_imag = -jnp.einsum("mj,szxj->szxm", sine_y, density, precision=highest)
    plane_real = jnp.einsum("mj,szjy->szmy", cosine_x, along_real, precision=highest) + jnp.einsum(
        "mj,szjy->szmy", sine_x, along_imag, precision=highest
    )
    plane_imag = jnp.einsum("mj,szjy->szmy", cosine_x, along_imag, precision=highest) - jnp.einsum(
        "mj,szjy->szmy", sine_x, along_real, precision=highest
    )
    dens_col, real_col, imag_col = to_columns((density, plane_real, plane_imag), 2)
    gradz_col = jnp.einsum("ik,skxy->sixy", deriv_z, dens_col, precision=highest)
    grad_z = exchange([gradz_col.reshape(128, 2, 128)], 3)[0].transpose(1, 0, 2)[None]
    gradient_square, xc_stress = xc_terms(density, grad_x, grad_y, grad_z, cell_count)
    spec_real = (
        jnp.einsum("mj,jxy->mxy", cosine_z, real_col[0], precision=highest)
        + jnp.einsum("mj,jxy->mxy", sine_z, imag_col[0], precision=highest)
    ) / cell_count
    spec_imag = (
        jnp.einsum("mj,jxy->mxy", cosine_z, imag_col[0], precision=highest)
        - jnp.einsum("mj,jxy->mxy", sine_z, real_col[0], precision=highest)
    ) / cell_count
    total_real, total_imag = packed_total((spec_real, spec_imag), "spin")
    local_rows = real_col.shape[2]
    first_column = lax.axis_index(BAND) * local_rows
    freq_z = frequencies(NZ)[:, None, None]
    freq_x = lax.dynamic_slice_in_dim(frequencies(NX), first_column, local_rows, 0)[None, :, None]
    freq_y = frequencies(NY)[None, None, :]
    length_sq = freq_x * freq_x + freq_y * freq_y + freq_z * freq_z
    positive = length_sq > 0
    inverse = jnp.where(positive, 1.0 / jnp.where(positive, length_sq, 1.0), 0.0)
    hartree_weight = 4.0 * jnp.pi * (total_real * total_real + total_imag * total_imag) * inverse
    diagonal = jnp.array([1.0, 1.0, 1.0, 0.0, 0.0, 0.0], jnp.float32)
    hartree_stress = 2.0 * six_sums(
        hartree_weight * inverse, freq_x, freq_y, freq_z
    ) - diagonal * jnp.sum(hartree_weight)
    local_weight = 2.0 * (total_real * local_factor[0] + total_imag * local_factor[1])
    local_stress = six_sums(local_weight, freq_x, freq_y, freq_z)
    spin_share = 1.0 / lax.axis_size("spin")
    partial_stress = spin_share * (hartree_stress + local_stress) + xc_stress
    stress = total(tile + jnp.pad(partial_stress[:, None], ((0, 2), (0, 127))))
    return (stress, kinetic_density.reshape(-1), gradient_square)


def solution(mesh):
    finer = Mesh(
        mesh.devices.reshape(2, 8, 4, 2, mesh.shape["spin"]),
        ("band_0", "band_1", "band_2", "band_3", "spin"),
    )
    return jax.shard_map(
        shards,
        mesh=finer,
        in_specs=(
            P("spin", None, BAND, None),
            P("spin", BAND),
            P(None, BAND_SPIN),
            P("spin", BAND, None, None),
            P(None, None, BAND, None),
        ),
        out_specs=(P(), P(BAND_SPIN), P("spin", BAND, None, None)),
        check_vma=False,
    )
```

```python
import jax
import jax.numpy as jnp
import numpy as np
from jax import lax
from jax.experimental import pallas as pl
from jax.experimental.pallas import tpu as pltpu
from jax.sharding import PartitionSpec as P

NPW = 524288
NX = 128
NY = 128
NZ = 256
CELLS = NX * NY * NZ
MESH = pl.DeviceIdType.MESH
F32, BF16 = jnp.float32, jnp.bfloat16

occupation_unit = 1000.0
kpoint = (0.25, 0.125, 0.375)
spacing = 0.25


def derivative_table(length):
    apart = np.arange(length)[:, None] - np.arange(length)[None, :]
    angles = np.pi / length * np.where(apart == 0, 1, apart)
    return np.where(apart == 0, 0.0, 0.5 * (1.0 - 2.0 * (apart % 2)) * np.cos(angles) / np.sin(angles))


def fourier_tables(length):
    index = np.arange(length)
    phases = (index[:, None] * index[None, :]) % length * (2.0 * np.pi / length)
    return np.cos(phases), np.sin(phases)


def halves(table):
    table = np.asarray(table, np.float32)
    high = table.astype(BF16)
    return np.stack([high, (table - high.astype(np.float32)).astype(BF16)])


def tables():
    cos_y, sin_y = fourier_tables(NY)
    cos_x, sin_x = fourier_tables(NX)
    cos_z, sin_z = fourier_tables(NZ)
    lo, hi = slice(0, 64), slice(64, 128)
    re, im = cos_y, -sin_y
    along_y = np.concatenate(
        [re[:, lo], im[:, lo], re[:, hi], im[:, hi], im[:, lo], -re[:, lo], im[:, hi], -re[:, hi], derivative_table(NY).T],
        axis=1,
    )
    along_x = np.concatenate([cos_x, sin_x], axis=1)
    along_z = np.concatenate([cos_z, sin_z], axis=1)
    return [halves(t) for t in (along_y, along_x, along_z, derivative_table(NX), derivative_table(NZ))]


def split(value):
    high = value.astype(BF16)
    return high, (value - high.astype(F32)).astype(BF16)


def product(left, right):
    def dot(a, b):
        return jnp.dot(a, b, preferred_element_type=F32)

    return dot(left[0], right[0]) + (dot(left[0], right[1]) + dot(left[1], right[0]))


def pair(table):
    return table[0], table[1]


def stress_kernel(
    occ, miller, coef_any, dens_any, factor_any, ty_any, tx_any, tz_any, dx_any, dz_any,
    stress, density_out, square_out,
    coef, dens, factor, ty, tx, tz, dx, dz,
    sn, rn, gz, rg, sp, rsp,
    part, twin, qa, qb, ra, rb, a1, b1, ra2, rb2, ab, rz, tmp,
    held, tot_z, tot_p,
    gradx, grady, far, lsem, ssem, rsem, bulk_s, bulk_r, tsem_s, tsem_r,
):
    band, s = lax.axis_index("band"), lax.axis_index("spin")
    x_lo, z, y, c = band // 64, lax.rem(band // 8, 8), lax.rem(band // 2, 4), lax.rem(band, 2)
    x = s * 2 + x_lo
    other = 1 - c

    def at(x_=None, z_=None, y_=None, c_=None):
        x_ = x if x_ is None else x_
        z_ = z if z_ is None else z_
        y_ = y if y_ is None else y_
        c_ = c if c_ is None else c_
        return {"band": ((lax.rem(x_, 2) * 8 + z_) * 4 + y_) * 2 + c_, "spin": x_ // 2}

    x_peers = [lax.rem(x + d, 4) for d in (1, 2, 3)]
    y_peers = [lax.rem(y + d, 4) for d in (1, 2, 3)]
    z_peers = [lax.rem(z + d, 8) for d in range(1, 8)]
    plane = [
        at(x_=lax.rem(x + d // 8, 4), y_=lax.rem(y + d // 2, 4), c_=lax.rem(c + d, 2)) for d in range(1, 32)
    ]

    locals_ = []
    for k, (src, dst) in enumerate(
        ((dens_any, dens), (ty_any, ty), (tx_any, tx), (dx_any, dx), (coef_any, coef), (dz_any, dz), (tz_any, tz), (factor_any, factor))
    ):
        copy = pltpu.make_async_copy(src, dst, lsem.at[k])
        copy.start()
        locals_.append(copy)
    load_dens, load_ty, load_tx, load_dx, load_coef, load_dz, load_tz, load_factor = locals_
    barrier = pltpu.get_barrier_semaphore()
    for p in z_peers:
        pl.semaphore_signal(barrier, inc=1, device_id=at(z_=p), device_id_type=MESH)
    for peer in plane:
        pl.semaphore_signal(barrier, inc=1, device_id=peer, device_id_type=MESH)

    pending = []

    def send(src, dst, k, peer):
        copy = pltpu.make_async_remote_copy(
            src_ref=src, dst_ref=dst, send_sem=ssem.at[k], recv_sem=rsem.at[k], device_id=peer, device_id_type=MESH
        )
        copy.start()
        pending.append(copy)
        return copy

    load_dens.wait()
    sn_flat = sn.reshape(256, 128)
    for zz in range(2):
        sn_flat[pl.ds(zz, 128, stride=2), :] = dens[zz]

    load_coef.wait()
    w0 = jnp.full((64, 128), occ[0, 0].astype(F32)) / occupation_unit
    w1 = jnp.full((64, 128), occ[0, 1].astype(F32)) / occupation_unit

    def squares(i, carry):
        rows = pl.ds(pl.multiple_of(i * 128, 128), 128)
        re = coef[0, rows, :].astype(F32)
        im = coef[1, rows, :].astype(F32)
        tmp[...] = re * re + im * im
        both = w0 * tmp[pl.ds(0, 64, stride=2), :] + w1 * tmp[pl.ds(1, 64, stride=2), :]
        part[i] = both.reshape(2, 32, 128)
        return carry

    lax.fori_loop(0, 64, squares, 0)

    pl.semaphore_wait(barrier, 38)
    for p in z_peers:
        pl.semaphore_signal(far, inc=1, device_id=at(z_=p), device_id_type=MESH)
    twins = [
        send(part.at[pl.ds(q * 16, 16), other], twin.at[pl.ds(q * 16, 16)], q, at(c_=other)) for q in range(4)
    ]

    load_ty.wait()
    load_tx.wait()
    load_dx.wait()
    rows = split(dens[...].reshape(256, 128))
    from_y = product(rows, pair(ty))
    wide = split(jnp.concatenate([dens[0], dens[1]], axis=1))
    gx = product(pair(dx), wide)
    sp_flat = sp.reshape(512, 128)
    for zz in range(2):
        mine = from_y[zz * 128 : zz * 128 + 128]
        grady[zz] = mine[:, 512:640]
        gradx[zz] = gx[:, zz * 128 : zz * 128 + 128]
        turned = product(pair(tx), split(jnp.concatenate([mine[:, 0:256], mine[:, 256:512]], axis=0)))
        for half in range(2):
            sp_flat[pl.ds(half * 256 + zz, 128, stride=2), :] = turned[:, half * 128 : half * 128 + 128]

    pl.semaphore_wait(far, 7)

    def push_density(d, carry):
        t = lax.rem(band + d, 128)
        pltpu.make_async_remote_copy(
            src_ref=sn.at[t], dst_ref=rn.at[band], send_sem=bulk_s.at[0], recv_sem=bulk_r.at[0],
            device_id={"band": t}, device_id_type=MESH,
        ).start()
        return carry

    lax.fori_loop(1, 128, push_density, 0)
    rn[band] = sn[band]

    for q in range(4):
        twins[q].wait_recv()

        def add_twin(i, carry):
            x_lo_, zz, yy = i // 32, lax.rem(i // 4, 8), lax.rem(i, 4)
            v = part[i, c] + twin[i]
            for x_hi in range(2):
                pos = x_hi * 2 + x_lo_
                qa[pos, yy * 8 + zz] = v[x_hi * 16 : x_hi * 16 + 8]
                qb[yy, pos * 8 + zz] = v[x_hi * 16 + 8 : x_hi * 16 + 16]
            return carry

        lax.fori_loop(q * 16, q * 16 + 16, add_twin, 0)
    first_a = [send(qa.at[p], ra.at[d], 4 + d, at(x_=p)) for d, p in enumerate(x_peers)]
    first_b = [send(qb.at[p], rb.at[d], 7 + d, at(y_=p)) for d, p in enumerate(y_peers)]

    me = s * 128 + band

    def push_spectrum(d, carry):
        t = lax.rem(me + d, 256)
        pltpu.make_async_remote_copy(
            src_ref=sp.at[t], dst_ref=rsp.at[me], send_sem=bulk_s.at[1], recv_sem=bulk_r.at[1],
            device_id={"band": lax.rem(t, 128), "spin": t // 128}, device_id_type=MESH,
        ).start()
        return carry

    lax.fori_loop(1, 256, push_spectrum, 0)
    rsp[me] = sp[me]

    load_dz.wait()
    all_n = rn.at[pl.ds(0, 127)]
    pltpu.make_async_copy(all_n, all_n, bulk_r.at[0]).wait()
    gz.reshape(256, 128)[...] = product(pair(dz), split(rn.reshape(256, 128)[...]))

    def push_back(d, carry):
        t = lax.rem(band + d, 128)
        pltpu.make_async_remote_copy(
            src_ref=gz.at[t], dst_ref=rg.at[band], send_sem=bulk_s.at[2], recv_sem=bulk_r.at[2],
            device_id={"band": t}, device_id_type=MESH,
        ).start()
        return carry

    lax.fori_loop(1, 128, push_back, 0)
    rg[band] = gz[band]

    for copy in first_a:
        copy.wait_recv()
    for t in range(4):
        sub = pl.ds(t * 8, 8)
        a1[t] = (qa[x, sub] + ra[0, sub]) + (ra[1, sub] + ra[2, sub])
    second_a = [send(a1.at[p], ra2.at[d], 10 + d, at(y_=p)) for d, p in enumerate(y_peers)]
    for copy in first_b:
        copy.wait_recv()
    for t in range(4):
        sub = pl.ds(t * 8, 8)
        b1[t] = (qb[y, sub] + rb[0, sub]) + (rb[1, sub] + rb[2, sub])
    second_b = [send(b1.at[p], rb2.at[d], 13 + d, at(x_=p)) for d, p in enumerate(x_peers)]

    load_factor.wait()
    load_tz.wait()
    lane = lax.broadcasted_iota(jnp.int32, (256, 128), 1)
    row = lax.broadcasted_iota(jnp.int32, (256, 128), 0)
    low = lane < 64
    unit_x, unit_y, unit_z = 2.0 * np.pi / NX, 2.0 * np.pi / NY, 2.0 * np.pi / NZ
    ky = jnp.where(low, lane, lane - 64) - 64 * s
    fy = unit_y * ky.astype(F32)
    fz = unit_z * jnp.where(row >= NZ // 2, row - NZ, row).astype(F32)
    fx = unit_x * jnp.full((1, 128), jnp.where(band >= NX // 2, band - NX, band).astype(F32))
    length_sq = fx * fx + fy * fy + fz * fz
    positive = length_sq > 0
    inverse = jnp.where(positive, 1.0 / jnp.where(positive, length_sq, 1.0), 0.0)
    f0, f1 = factor[0], factor[1]
    first = jnp.where(s == 0, f0, pltpu.roll(f0, 64, 1))
    second = jnp.where(s == 0, pltpu.roll(f1, 64, 1), f1)
    local = 2.0 * jnp.where(low, first, second)

    all_sp = rsp.at[pl.ds(0, 255)]
    pltpu.make_async_copy(all_sp, all_sp, bulk_r.at[1]).wait()
    rsp_flat = rsp.reshape(512, 128)
    planes = (rsp_flat[0:256] + rsp_flat[256:512]) * (1.0 / CELLS)
    crossed = pltpu.roll(planes, 64, 1)
    crossed = jnp.where(low, crossed, -crossed)
    spectrum = product(pair(tz), split(jnp.concatenate([planes, crossed], axis=0)))
    hartree = (4.0 * np.pi) * (spectrum * spectrum) * inverse
    weighting = 2.0 * hartree * inverse + spectrum * local

    def down(value):
        return jnp.sum(value, axis=0, keepdims=True)

    sum_h = down(hartree)
    sum_1, sum_z, sum_zz = down(weighting), down(weighting * fz), down(weighting * fz * fz)
    fy1 = fy[0:1]
    spectral = [
        fx * fx * sum_1 - sum_h, fy1 * fy1 * sum_1 - sum_h, sum_zz - sum_h, fy1 * sum_z, fx * sum_z, fx * fy1 * sum_1
    ]

    for copy in second_a:
        copy.wait_recv()
    ab[:, 0] = (a1[y] + ra2[0]) + (ra2[1] + ra2[2])
    for copy in second_b:
        copy.wait_recv()
    ab[:, 1] = (b1[x] + rb2[0]) + (rb2[1] + rb2[2])
    last = [send(ab.at[p], rz.at[d], 16 + d, at(z_=p)) for d, p in enumerate(z_peers)]

    pltpu.make_async_copy(all_n, rg.at[pl.ds(0, 127)], bulk_r.at[2]).wait()
    rg_flat = rg.reshape(256, 128)
    xc = [jnp.zeros((1, 128), F32)] * 6
    pairs = ((0, 0), (1, 1), (2, 2), (1, 2), (0, 2), (0, 1))
    for zz in range(2):
        n = dens[zz]
        grads = (gradx[zz], grady[zz], rg_flat[pl.ds(zz, 128, stride=2), :])
        square = grads[0] * grads[0] + grads[1] * grads[1] + grads[2] * grads[2]
        square_out[zz] = square
        room = 4.0 * n * n + 1.0
        kernel = jnp.exp(jnp.log(n) * (-1.0 / 3.0)) * room / (room + square)
        scaled = [kernel * g for g in grads]
        xc = [t + down(scaled[a] * grads[b]) for t, (a, b) in zip(xc, pairs)]

    g = [spacing * (miller[a].astype(F32) + kpoint[a]) for a in range(3)]
    for copy in last:
        copy.wait_recv()
    weight = ab[z]
    for d in range(7):
        weight = weight + rz[d]
    weight = weight.reshape(16, 128)
    density_out[...] = 0.5 * (g[0] * g[0] + g[1] * g[1] + g[2] * g[2]) * weight
    kinetic = [down(weight * g[a] * g[b]) for a, b in pairs]
    lines = [spectral[a] - kinetic[a] * (1.0 / NPW) - xc[a] * (1.0 / CELLS) for a in range(6)]
    held[0] = jnp.concatenate(lines + [jnp.zeros((2, 128), F32)], axis=0)

    plane_me = (x * 4 + y) * 2 + c
    stages = ((tot_z, z, [at(z_=p) for p in z_peers], 8), (tot_p, plane_me, plane, 32))
    k = 0
    for stage, (slots, mine, peers, count) in enumerate(stages):
        copies = []
        for peer in peers:
            copy = pltpu.make_async_remote_copy(
                src_ref=held.at[stage], dst_ref=slots.at[mine], send_sem=tsem_s.at[k], recv_sem=tsem_r.at[k],
                device_id=peer, device_id_type=MESH,
            )
            copy.start()
            copies.append(copy)
            k += 1
        slots[mine] = held[stage]
        for copy in copies:
            copy.wait_recv()
        pending += copies
        level = [slots[j] for j in range(count)]
        while len(level) > 1:
            level = [level[j] + level[j + 1] for j in range(0, len(level), 2)]
        if stage == 0:
            held[1] = level[0]
    for a in range(6):
        stress[a] = jnp.sum(level[0][a : a + 1, :])

    for copy in pending:
        copy.wait_send()
    for k, ref in ((0, all_n), (1, all_sp), (2, all_n)):
        pltpu.make_async_copy(ref, ref, bulk_s.at[k]).wait()


def shards(coefficients, occupation, miller, density, local_factor):
    pairs = coefficients[0].reshape(2, 2, NPW // 128, 128).transpose(0, 2, 1, 3).reshape(2, NPW // 64, 128)
    ty, tx, tz, dx, dz = [jnp.asarray(t) for t in tables()]
    vmem, smem, far = (pl.BlockSpec(memory_space=m) for m in (pltpu.VMEM, pltpu.SMEM, pltpu.HBM))
    held = [(pairs.shape, BF16), ((2, 128, 128), F32), ((2, 256, 128), F32)] + [(t.shape, BF16) for t in (ty, tx, tz, dx, dz)]
    scratch = held + [
        (shape, F32)
        for shape in (
            (128, 2, 128), (128, 2, 128), (128, 2, 128), (128, 2, 128), (256, 2, 128), (256, 2, 128),
            (64, 2, 32, 128), (64, 32, 128), (4, 32, 8, 128), (4, 32, 8, 128), (3, 32, 8, 128), (3, 32, 8, 128),
            (4, 8, 8, 128), (4, 8, 8, 128), (3, 8, 8, 128), (3, 8, 8, 128), (8, 2, 8, 128), (7, 2, 8, 128), (128, 128),
            (2, 8, 128), (8, 8, 128), (32, 8, 128),
            (2, 128, 128), (2, 128, 128),
        )
    ]
    dma = pltpu.SemaphoreType.DMA
    stress, kinetic_density, square = pl.pallas_call(
        stress_kernel,
        out_shape=(
            jax.ShapeDtypeStruct((6,), F32),
            jax.ShapeDtypeStruct((16, 128), F32),
            jax.ShapeDtypeStruct((2, 128, 128), F32),
        ),
        in_specs=[smem, vmem] + [far] * 8,
        out_specs=(smem, vmem, vmem),
        scratch_shapes=[pltpu.VMEM(*one) for one in scratch]
        + [pltpu.SemaphoreType.REGULAR, dma((8,)), dma((23,)), dma((23,)), dma((3,)), dma((3,)), dma((38,)), dma((38,))],
        compiler_params=pltpu.CompilerParams(collective_id=0, has_side_effects=True),
    )(
        occupation, miller.reshape(3, 16, 128), pairs, density[0], local_factor.reshape(2, 256, 128), ty, tx, tz, dx, dz
    )
    return (stress, kinetic_density.reshape(-1), square[None])


def solution(mesh):
    return jax.shard_map(
        shards,
        mesh=mesh,
        in_specs=(
            P("spin", None, "band", None),
            P("spin", "band"),
            P(None, ("band", "spin")),
            P("spin", "band", None, None),
            P(None, None, "band", None),
        ),
        out_specs=(P(), P(("band", "spin")), P("spin", "band", None, None)),
        check_vma=False,
    )
```

```python
import jax
import jax.numpy as jnp
import numpy as np
from jax import lax
from jax.experimental import pallas as pl
from jax.experimental.pallas import tpu as pltpu
from jax.sharding import PartitionSpec as P

NPW = 524288
NX = 128
NY = 128
NZ = 256
CELLS = NX * NY * NZ
SPLIT = 96
MESH = pl.DeviceIdType.MESH
F32, BF16 = jnp.float32, jnp.bfloat16

occupation_unit = 1000.0
kpoint = (0.25, 0.125, 0.375)
spacing = 0.25


def derivative_table(length):
    apart = np.arange(length)[:, None] - np.arange(length)[None, :]
    angles = np.pi / length * np.where(apart == 0, 1, apart)
    return np.where(apart == 0, 0.0, 0.5 * (1.0 - 2.0 * (apart % 2)) * np.cos(angles) / np.sin(angles))


def fourier_tables(length):
    index = np.arange(length)
    phases = (index[:, None] * index[None, :]) % length * (2.0 * np.pi / length)
    return np.cos(phases), np.sin(phases)


def halves(table):
    table = np.asarray(table, np.float32)
    high = table.astype(BF16)
    return np.stack([high, (table - high.astype(np.float32)).astype(BF16)])


def tables():
    cos_y, sin_y = fourier_tables(NY)
    cos_x, sin_x = fourier_tables(NX)
    cos_z, sin_z = fourier_tables(NZ)
    lo, hi = slice(0, 64), slice(64, 128)
    re, im = cos_y, -sin_y
    along_y = np.concatenate(
        [re[:, lo], im[:, lo], re[:, hi], im[:, hi], im[:, lo], -re[:, lo], im[:, hi], -re[:, hi], derivative_table(NY).T],
        axis=1,
    )
    along_x = np.concatenate([cos_x, sin_x], axis=1)
    along_z = np.concatenate([cos_z, sin_z], axis=1)
    return [halves(t) for t in (along_y, along_x, along_z, derivative_table(NX), derivative_table(NZ))]


def split(value):
    high = value.astype(BF16)
    return high, (value - high.astype(F32)).astype(BF16)


def product(left, right):
    def dot(a, b):
        return jnp.dot(a, b, preferred_element_type=F32)

    return dot(left[0], right[0]) + (dot(left[0], right[1]) + dot(left[1], right[0]))


def pair(table):
    return table[0], table[1]


def stress_kernel(
    occ_any, miller_any, coef_any, dens_any, factor_any, ty_any, tx_any, tz_any, dx_any, dz_any,
    totals_out, density_out, square_out,
    occ, miller, coef, dens, factor, ty, tx, tz, dx, dz,
    sn, rn, gz, rg, sp, rsp,
    part, twin, qa, qb, ra, rb, ha, hb, a1, b1, ra2, rb2, ab, rz, tmp,
    held, tot_z, tot_p, density, square_held,
    gradx, grady, far, lsem, osem, ssem, rsem, bulk_s, bulk_r, tsem_s, tsem_r,
):
    band, s = lax.axis_index("band"), lax.axis_index("spin")
    x_lo, z, y, c = band // 64, lax.rem(band // 8, 8), lax.rem(band // 2, 4), lax.rem(band, 2)
    x = s * 2 + x_lo
    other = 1 - c

    def at(x_=None, z_=None, y_=None, c_=None):
        x_ = x if x_ is None else x_
        z_ = z if z_ is None else z_
        y_ = y if y_ is None else y_
        c_ = c if c_ is None else c_
        return {"band": ((lax.rem(x_, 2) * 8 + z_) * 4 + y_) * 2 + c_, "spin": x_ // 2}

    x_peers = [lax.rem(x + d, 4) for d in (1, 2, 3)]
    y_peers = [lax.rem(y + d, 4) for d in (1, 2, 3)]
    z_peers = [lax.rem(z + d, 8) for d in range(1, 8)]
    plane = [
        at(x_=lax.rem(x + d // 8, 4), y_=lax.rem(y + d // 2, 4), c_=lax.rem(c + d, 2)) for d in range(1, 32)
    ]

    def load(src, dst, k):
        copy = pltpu.make_async_copy(src, dst, lsem.at[k])
        copy.start()
        return copy

    load_occ = load(occ_any, occ, 0)
    load_coef = [
        load(coef_any.at[:, pl.ds(q * 2048, 2048)], coef.at[:, pl.ds(q * 2048, 2048)], 1 + q) for q in range(4)
    ]
    load_dens, load_ty, load_tx, load_dx, load_dz, load_tz, load_factor, load_miller = [
        load(src, dst, 5 + k)
        for k, (src, dst) in enumerate(
            ((dens_any, dens), (ty_any, ty), (tx_any, tx), (dx_any, dx), (dz_any, dz), (tz_any, tz),
             (factor_any, factor), (miller_any, miller))
        )
    ]
    barrier = pltpu.get_barrier_semaphore()
    for p in z_peers:
        pl.semaphore_signal(barrier, inc=1, device_id=at(z_=p), device_id_type=MESH)
    for peer in plane:
        pl.semaphore_signal(barrier, inc=1, device_id=peer, device_id_type=MESH)

    pending = []

    def send(src, dst, k, peer):
        copy = pltpu.make_async_remote_copy(
            src_ref=src, dst_ref=dst, send_sem=ssem.at[k], recv_sem=rsem.at[k], device_id=peer, device_id_type=MESH
        )
        copy.start()
        pending.append(copy)
        return copy

    load_occ.wait()
    w0 = jnp.full((64, 128), occ[0, 0].astype(F32)) / occupation_unit
    w1 = jnp.full((64, 128), occ[0, 1].astype(F32)) / occupation_unit

    def squares(i, carry):
        for u in range(2):
            rows = pl.ds(pl.multiple_of(i * 256 + u * 128, 128), 128)
            re = coef[0, rows, :].astype(F32)
            im = coef[1, rows, :].astype(F32)
            tmp[u] = re * re + im * im
            both = w0 * tmp[u, pl.ds(0, 64, stride=2), :] + w1 * tmp[u, pl.ds(1, 64, stride=2), :]
            part[i * 2 + u] = both.reshape(2, 32, 128)
        return carry

    for q in range(4):
        load_coef[q].wait()
        lax.fori_loop(q * 8, q * 8 + 8, squares, 0)

    pl.semaphore_wait(barrier, 38)
    twins = [
        send(part.at[pl.ds(q * 16, 16), other], twin.at[pl.ds(q * 16, 16)], q, at(c_=other)) for q in range(4)
    ]
    for p in z_peers:
        pl.semaphore_signal(far, inc=1, device_id=at(z_=p), device_id_type=MESH)

    load_dens.wait()
    sn_flat = sn.reshape(256, 128)
    for zz in range(2):
        sn_flat[pl.ds(zz, 128, stride=2), :] = dens[zz]

    load_ty.wait()
    load_tx.wait()
    load_dx.wait()
    rows = split(dens[...].reshape(256, 128))
    from_y = product(rows, pair(ty))
    wide = split(jnp.concatenate([dens[0], dens[1]], axis=1))
    gx = product(pair(dx), wide)
    sp_flat = sp.reshape(512, 128)
    for zz in range(2):
        mine = from_y[zz * 128 : zz * 128 + 128]
        grady[zz] = mine[:, 512:640]
        gradx[zz] = gx[:, zz * 128 : zz * 128 + 128]
        turned = product(pair(tx), split(jnp.concatenate([mine[:, 0:256], mine[:, 256:512]], axis=0)))
        for half in range(2):
            sp_flat[pl.ds(half * 256 + zz, 128, stride=2), :] = turned[:, half * 128 : half * 128 + 128]

    for q in range(4):
        twins[q].wait_recv()

        def add_twin(j, carry):
            for u in range(4):
                i = j * 4 + u
                x_lo_, zz, yy = i // 32, lax.rem(i // 4, 8), u
                v = part[i, c] + twin[i]
                for x_hi in range(2):
                    pos = x_hi * 2 + x_lo_
                    qa[pos, yy * 8 + zz] = v[x_hi * 16 : x_hi * 16 + 8]
                    qb[yy, pos * 8 + zz] = v[x_hi * 16 + 8 : x_hi * 16 + 16]
            return carry

        lax.fori_loop(q * 4, q * 4 + 4, add_twin, 0)
    top, low_half = pl.ds(0, 16), pl.ds(16, 16)
    rings = (
        (qa, ra, ha, x_peers, lambda p: at(x_=p), 4),
        (qb, rb, hb, y_peers, lambda p: at(y_=p), 10),
    )
    relays, firsts = [], []
    for own, got, half, (right, across, left), where, k in rings:
        relays.append(
            (
                send(own.at[across, top], half.at[0], k, where(right)),
                send(own.at[across, low_half], half.at[1], k + 1, where(left)),
            )
        )
    for own, got, half, (right, across, left), where, k in rings:
        firsts.append(
            [
                send(own.at[right, low_half], got.at[0, low_half], k + 2, where(right)),
                send(own.at[left, top], got.at[1, top], k + 3, where(left)),
            ]
        )

    pl.semaphore_wait(far, 7)

    def push_density(d, carry):
        t = lax.rem(band + d, 128)
        pltpu.make_async_remote_copy(
            src_ref=sn.at[t], dst_ref=rn.at[band], send_sem=bulk_s.at[0], recv_sem=bulk_r.at[0],
            device_id={"band": t}, device_id_type=MESH,
        ).start()
        return carry

    lax.fori_loop(1, 128, push_density, 0)
    rn[band] = sn[band]

    me = s * 128 + band

    def push_spectrum(d, carry):
        t = lax.rem(me + d, 256)
        pltpu.make_async_remote_copy(
            src_ref=sp.at[t], dst_ref=rsp.at[me], send_sem=bulk_s.at[1], recv_sem=bulk_r.at[1],
            device_id={"band": lax.rem(t, 128), "spin": t // 128}, device_id_type=MESH,
        ).start()
        return carry

    lax.fori_loop(1, SPLIT, push_spectrum, 0)
    for (own, got, half, (right, across, left), where, k), (to_right, to_left), first in zip(rings, relays, firsts):
        to_right.wait_recv()
        half[2] = own[right, top] + half[0]
        first.append(send(half.at[2], got.at[0, top], k + 4, where(right)))
        to_left.wait_recv()
        half[3] = own[left, low_half] + half[1]
        first.append(send(half.at[3], got.at[1, low_half], k + 5, where(left)))
    lax.fori_loop(SPLIT, 256, push_spectrum, 0)
    rsp[me] = sp[me]

    load_dz.wait()
    all_n = rn.at[pl.ds(0, 127)]
    pltpu.make_async_copy(all_n, all_n, bulk_r.at[0]).wait()
    gz.reshape(256, 128)[...] = product(pair(dz), split(rn.reshape(256, 128)[...]))

    def push_back(d, carry):
        t = lax.rem(band + d, 128)
        pltpu.make_async_remote_copy(
            src_ref=gz.at[t], dst_ref=rg.at[band], send_sem=bulk_s.at[2], recv_sem=bulk_r.at[2],
            device_id={"band": t}, device_id_type=MESH,
        ).start()
        return carry

    lax.fori_loop(1, 128, push_back, 0)
    rg[band] = gz[band]

    for copy in firsts[0]:
        copy.wait_recv()
    for t in range(4):
        sub = pl.ds(t * 8, 8)
        a1[t] = qa[x, sub] + (ra[0, sub] + ra[1, sub])
    second_a = [send(a1.at[p], ra2.at[d], 16 + d, at(y_=p)) for d, p in enumerate(y_peers)]
    for copy in firsts[1]:
        copy.wait_recv()
    for t in range(4):
        sub = pl.ds(t * 8, 8)
        b1[t] = qb[y, sub] + (rb[0, sub] + rb[1, sub])
    second_b = [send(b1.at[p], rb2.at[d], 19 + d, at(x_=p)) for d, p in enumerate(x_peers)]

    load_factor.wait()
    load_tz.wait()
    lane = lax.broadcasted_iota(jnp.int32, (256, 128), 1)
    row = lax.broadcasted_iota(jnp.int32, (256, 128), 0)
    low = lane < 64
    unit_x, unit_y, unit_z = 2.0 * np.pi / NX, 2.0 * np.pi / NY, 2.0 * np.pi / NZ
    ky = jnp.where(low, lane, lane - 64) - 64 * s
    fy = unit_y * ky.astype(F32)
    fz = unit_z * jnp.where(row >= NZ // 2, row - NZ, row).astype(F32)
    fx = unit_x * jnp.full((1, 128), jnp.where(band >= NX // 2, band - NX, band).astype(F32))
    length_sq = fx * fx + fy * fy + fz * fz
    positive = length_sq > 0
    inverse = jnp.where(positive, 1.0 / jnp.where(positive, length_sq, 1.0), 0.0)
    f0, f1 = factor[0], factor[1]
    first = jnp.where(s == 0, f0, pltpu.roll(f0, 64, 1))
    second = jnp.where(s == 0, pltpu.roll(f1, 64, 1), f1)
    local = 2.0 * jnp.where(low, first, second)

    all_sp = rsp.at[pl.ds(0, 255)]
    pltpu.make_async_copy(all_sp, all_sp, bulk_r.at[1]).wait()
    rsp_flat = rsp.reshape(512, 128)
    planes = (rsp_flat[0:256] + rsp_flat[256:512]) * (1.0 / CELLS)
    crossed = pltpu.roll(planes, 64, 1)
    crossed = jnp.where(low, crossed, -crossed)
    spectrum = product(pair(tz), split(jnp.concatenate([planes, crossed], axis=0)))
    hartree = (4.0 * np.pi) * (spectrum * spectrum) * inverse
    weighting = 2.0 * hartree * inverse + spectrum * local

    def down(value):
        return jnp.sum(value, axis=0, keepdims=True)

    sum_h = down(hartree)
    sum_1, sum_z, sum_zz = down(weighting), down(weighting * fz), down(weighting * fz * fz)
    fy1 = fy[0:1]
    spectral = [
        fx * fx * sum_1 - sum_h, fy1 * fy1 * sum_1 - sum_h, sum_zz - sum_h, fy1 * sum_z, fx * sum_z, fx * fy1 * sum_1
    ]

    for copy in second_a:
        copy.wait_recv()
    ab[:, 0] = (a1[y] + ra2[0]) + (ra2[1] + ra2[2])
    for copy in second_b:
        copy.wait_recv()
    ab[:, 1] = (b1[x] + rb2[0]) + (rb2[1] + rb2[2])
    last = [send(ab.at[p], rz.at[d], 22 + d, at(z_=p)) for d, p in enumerate(z_peers)]

    pltpu.make_async_copy(all_n, rg.at[pl.ds(0, 127)], bulk_r.at[2]).wait()
    rg_flat = rg.reshape(256, 128)
    xc = [jnp.zeros((1, 128), F32)] * 6
    pairs = ((0, 0), (1, 1), (2, 2), (1, 2), (0, 2), (0, 1))
    for zz in range(2):
        n = dens[zz]
        grads = (gradx[zz], grady[zz], rg_flat[pl.ds(zz, 128, stride=2), :])
        square = grads[0] * grads[0] + grads[1] * grads[1] + grads[2] * grads[2]
        square_held[zz] = square
        room = 4.0 * n * n + 1.0
        kernel = jnp.exp(jnp.log(n) * (-1.0 / 3.0)) * room / (room + square)
        scaled = [kernel * g for g in grads]
        xc = [t + down(scaled[a] * grads[b]) for t, (a, b) in zip(xc, pairs)]

    store_square = pltpu.make_async_copy(square_held, square_out, osem.at[0])
    store_square.start()
    load_miller.wait()
    g = [spacing * (miller[:, a].astype(F32) + kpoint[a]) for a in range(3)]
    for copy in last:
        copy.wait_recv()
    weight = ab[z]
    for d in range(7):
        weight = weight + rz[d]
    weight = weight.reshape(16, 128)
    density[...] = 0.5 * (g[0] * g[0] + g[1] * g[1] + g[2] * g[2]) * weight
    kinetic = [down(weight * g[a] * g[b]) for a, b in pairs]
    lines = [spectral[a] - kinetic[a] * (1.0 / NPW) - xc[a] * (1.0 / CELLS) for a in range(6)]
    sums = jnp.sum(jnp.concatenate(lines + [jnp.zeros((2, 128), F32)], axis=0), axis=1, keepdims=True)
    diagonal = lax.broadcasted_iota(jnp.int32, (8, 128), 0) == lax.broadcasted_iota(jnp.int32, (8, 128), 1)
    held[0] = down(jnp.where(diagonal, sums, 0.0))

    plane_me = (x * 4 + y) * 2 + c
    stages = ((tot_z, z, [at(z_=p) for p in z_peers], 8), (tot_p, plane_me, plane, 32))
    k = 0
    for stage, (slots, mine, peers, count) in enumerate(stages):
        copies = []
        for peer in peers:
            copy = pltpu.make_async_remote_copy(
                src_ref=held.at[stage], dst_ref=slots.at[mine], send_sem=tsem_s.at[k], recv_sem=tsem_r.at[k],
                device_id=peer, device_id_type=MESH,
            )
            copy.start()
            copies.append(copy)
            k += 1
        slots[mine] = held[stage]
        if stage == 0:
            store_density = pltpu.make_async_copy(density, density_out, osem.at[1])
            store_density.start()
        for copy in copies:
            copy.wait_recv()
        pending += copies
        held[stage + 1] = down(slots.reshape(count, 128)[...])
    store_totals = pltpu.make_async_copy(held.at[2], totals_out, osem.at[2])
    store_totals.start()

    for copy in pending:
        copy.wait_send()
    for k, ref in ((0, all_n), (1, all_sp), (2, all_n)):
        pltpu.make_async_copy(ref, ref, bulk_s.at[k]).wait()
    store_square.wait()
    store_density.wait()
    store_totals.wait()


def emit_kernel(totals_any, density_any, square_any, stress_out, density_out, square_out, totals, stress, density, square, sem):
    into = [
        pltpu.make_async_copy(src, dst, sem.at[k])
        for k, (src, dst) in enumerate(((square_any, square), (density_any, density), (totals_any, totals)))
    ]
    for copy in into:
        copy.start()
    out = [
        pltpu.make_async_copy(src, dst, sem.at[3 + k])
        for k, (src, dst) in enumerate(((square, square_out), (density, density_out), (stress, stress_out)))
    ]
    for k in range(2):
        into[k].wait()
        out[k].start()
    into[2].wait()
    for a in range(6):
        stress[a] = totals[0, a]
    out[2].start()
    for copy in out:
        copy.wait()


def shards(coefficients, occupation, miller, density, local_factor):
    pairs = coefficients[0].reshape(2, 2, NPW // 128, 128).transpose(0, 2, 1, 3).reshape(2, NPW // 64, 128)
    ty, tx, tz, dx, dz = [jnp.asarray(t) for t in tables()]
    hbm = pl.BlockSpec(memory_space=pltpu.HBM)
    millers = miller.reshape(3, 16, 128).transpose(1, 0, 2)
    loaded = [(millers.shape, jnp.int32), (pairs.shape, BF16), ((2, 128, 128), F32), ((2, 256, 128), F32)]
    loaded += [(t.shape, BF16) for t in (ty, tx, tz, dx, dz)]
    scratch = loaded + [
        (shape, F32)
        for shape in (
            (128, 2, 128), (128, 2, 128), (128, 2, 128), (128, 2, 128), (256, 2, 128), (256, 2, 128),
            (64, 2, 32, 128), (64, 32, 128), (4, 32, 8, 128), (4, 32, 8, 128), (2, 32, 8, 128), (2, 32, 8, 128),
            (4, 16, 8, 128), (4, 16, 8, 128),
            (4, 8, 8, 128), (4, 8, 8, 128), (3, 8, 8, 128), (3, 8, 8, 128), (8, 2, 8, 128), (7, 2, 8, 128), (2, 128, 128),
            (3, 1, 128), (8, 1, 128), (32, 1, 128), (16, 128), (2, 128, 128),
            (2, 128, 128), (2, 128, 128),
        )
    ]
    dma = pltpu.SemaphoreType.DMA
    results = (
        jax.ShapeDtypeStruct((1, 128), F32),
        jax.ShapeDtypeStruct((16, 128), F32),
        jax.ShapeDtypeStruct((2, 128, 128), F32),
    )
    totals, kinetic_density, square = pl.pallas_call(
        stress_kernel,
        out_shape=results,
        in_specs=[hbm] * 10,
        out_specs=(hbm,) * 3,
        scratch_shapes=[pltpu.SMEM((1, 2), jnp.int32)]
        + [pltpu.VMEM(*one) for one in scratch]
        + [pltpu.SemaphoreType.REGULAR, dma((13,)), dma((3,)), dma((29,)), dma((29,)), dma((3,)), dma((3,))]
        + [dma((38,)), dma((38,))],
        compiler_params=pltpu.CompilerParams(collective_id=0, has_side_effects=True),
    )(occupation, millers, pairs, density[0], local_factor.reshape(2, 256, 128), ty, tx, tz, dx, dz)
    stress, kinetic_density, square = pl.pallas_call(
        emit_kernel,
        out_shape=(jax.ShapeDtypeStruct((6,), F32),) + results[1:],
        in_specs=[hbm] * 3,
        out_specs=(hbm,) * 3,
        scratch_shapes=[
            pltpu.SMEM((1, 128), F32),
            pltpu.SMEM((6,), F32),
            pltpu.VMEM((16, 128), F32),
            pltpu.VMEM((2, 128, 128), F32),
            dma((6,)),
        ],
    )(totals, kinetic_density, square)
    return (stress, kinetic_density.reshape(-1), square[None])


def solution(mesh):
    return jax.shard_map(
        shards,
        mesh=mesh,
        in_specs=(
            P("spin", None, "band", None),
            P("spin", "band"),
            P(None, ("band", "spin")),
            P("spin", "band", None, None),
            P(None, None, "band", None),
        ),
        out_specs=(P(), P(("band", "spin")), P("spin", "band", None, None)),
        check_vma=False,
    )
```

```python
import functools

import jax
import jax.numpy as jnp
import numpy as np
from jax import lax
from jax.experimental import pallas as pl
from jax.experimental.pallas import tpu as pltpu
from jax.sharding import PartitionSpec as P

NPW = 524288
NX = 128
NY = 128
NZ = 256
CELLS = NX * NY * NZ
MESH = pl.DeviceIdType.MESH
F32, BF16 = jnp.float32, jnp.bfloat16

occupation_unit = 1000.0
kpoint = (0.25, 0.125, 0.375)
spacing = 0.25


def derivative_table(length):
    apart = np.arange(length)[:, None] - np.arange(length)[None, :]
    angles = np.pi / length * np.where(apart == 0, 1, apart)
    return np.where(apart == 0, 0.0, 0.5 * (1.0 - 2.0 * (apart % 2)) * np.cos(angles) / np.sin(angles))


def fourier_tables(length):
    index = np.arange(length)
    phases = (index[:, None] * index[None, :]) % length * (2.0 * np.pi / length)
    return np.cos(phases), np.sin(phases)


def halves(table):
    table = np.asarray(table, np.float32)
    high = table.astype(BF16)
    return np.stack([high, (table - high.astype(np.float32)).astype(BF16)])


def tables():
    cos_y, sin_y = fourier_tables(NY)
    cos_x, sin_x = fourier_tables(NX)
    cos_z, sin_z = fourier_tables(NZ)
    lo, hi = slice(0, 64), slice(64, 128)
    re, im = cos_y, -sin_y
    along_y = np.concatenate(
        [re[:, lo], im[:, lo], re[:, hi], im[:, hi], im[:, lo], -re[:, lo], im[:, hi], -re[:, hi], derivative_table(NY).T],
        axis=1,
    )
    along_x = np.concatenate([cos_x, sin_x], axis=1)
    along_z = np.concatenate([cos_z, sin_z], axis=1)
    plane = np.concatenate([along_y, along_x, derivative_table(NX)], axis=1)
    column = np.concatenate([along_z, derivative_table(NZ)], axis=1)
    return [halves(t) for t in (plane, column)]


def split(value):
    high = value.astype(BF16)
    return high, (value - high.astype(F32)).astype(BF16)


def product(left, right):
    def dot(a, b):
        return jnp.dot(a, b, preferred_element_type=F32)

    return dot(left[0], right[0]) + (dot(left[0], right[1]) + dot(left[1], right[0]))


def pair(table, first, last):
    return table[0, :, first:last], table[1, :, first:last]


def stress_kernel(
    occ_any, miller_any, coef_any, dens_any, factor_any, plane_any, column_any,
    totals_out, density_out, square_out,
    occ, millers, coef, dens, far_plane, factor, in_plane, in_column,
    sn, rn, gz, rg, sp, rsp,
    part, twin, qa, qb, ra, rb, ha, hb, a1, b1, ra2, rb2, ab, rz, tmp,
    held, tot_z, tot_p, density, square_held,
    gradx, grady, far, lsem, osem, ssem, rsem, bulk_s, bulk_r,
):
    band, s = lax.axis_index("band"), lax.axis_index("spin")
    x_lo, z, y, c = band // 64, lax.rem(band // 8, 8), lax.rem(band // 2, 4), lax.rem(band, 2)
    x = s * 2 + x_lo
    other = 1 - c

    def at(x_=None, z_=None, y_=None, c_=None):
        x_ = x if x_ is None else x_
        z_ = z if z_ is None else z_
        y_ = y if y_ is None else y_
        c_ = c if c_ is None else c_
        return {"band": ((lax.rem(x_, 2) * 8 + z_) * 4 + y_) * 2 + c_, "spin": x_ // 2}

    x_peers = [lax.rem(x + d, 4) for d in (1, 2, 3)]
    y_peers = [lax.rem(y + d, 4) for d in (1, 2, 3)]
    z_peers = [lax.rem(z + d, 8) for d in range(1, 8)]
    plane = [
        at(x_=lax.rem(x + d // 8, 4), y_=lax.rem(y + d // 2, 4), c_=lax.rem(c + d, 2)) for d in range(1, 32)
    ]

    def load(src, dst, k):
        copy = pltpu.make_async_copy(src, dst, lsem.at[k])
        copy.start()
        return copy

    load_occ = load(occ_any, occ, 0)
    load_coef = [
        load(coef_any.at[:, pl.ds(q * 2048, 2048)], coef.at[:, pl.ds(q * 2048, 2048)], 1 + q) for q in range(4)
    ]
    barrier = pltpu.get_barrier_semaphore()
    for p in z_peers:
        pl.semaphore_signal(barrier, inc=1, device_id=at(z_=p), device_id_type=MESH)
    for peer in plane:
        pl.semaphore_signal(barrier, inc=1, device_id=peer, device_id_type=MESH)

    load_dens, load_plane, load_column, load_factor, load_miller = [
        load(src, dst, 5 + k)
        for k, (src, dst) in enumerate(
            ((dens_any, dens), (plane_any, in_plane), (column_any, in_column), (factor_any, factor),
             (miller_any, millers.at[z]))
        )
    ]
    def send(src, dst, k, peer):
        copy = pltpu.make_async_remote_copy(
            src_ref=src, dst_ref=dst, send_sem=ssem.at[0], recv_sem=rsem.at[k], device_id=peer, device_id_type=MESH
        )
        copy.start()
        return copy

    def arrived(ref, sem):
        pltpu.make_async_copy(ref, ref, sem).wait()

    load_occ.wait()
    w0 = jnp.full((64, 128), occ[0, 0].astype(F32)) / occupation_unit
    w1 = jnp.full((64, 128), occ[0, 1].astype(F32)) / occupation_unit

    def squares(i, carry):
        for u in range(2):
            rows = pl.ds(pl.multiple_of(i * 256 + u * 128, 128), 128)
            re = coef[0, rows, :].astype(F32)
            im = coef[1, rows, :].astype(F32)
            tmp[u] = re * re + im * im
            both = w0 * tmp[u, pl.ds(0, 64, stride=2), :] + w1 * tmp[u, pl.ds(1, 64, stride=2), :]
            part[i * 2 + u] = both.reshape(2, 32, 128)
        return carry

    for q in range(4):
        load_coef[q].wait()
        lax.fori_loop(q * 8, q * 8 + 8, squares, 0)

    pl.semaphore_wait(barrier, 38)
    twins = [
        send(part.at[pl.ds(q * 16, 16), other], twin.at[pl.ds(q * 16, 16)], q, at(c_=other)) for q in range(4)
    ]
    load_dens.wait()
    over_spin = send(dens.at[1 - s], far_plane, 4, at(x_=x_peers[1]))
    for p in z_peers:
        pl.semaphore_signal(far, inc=1, device_id=at(z_=p), device_id_type=MESH)
    load_miller.wait()
    for p in z_peers:
        send(millers.at[z], millers.at[z], 5, at(z_=p))

    sn_flat = sn.reshape(256, 128)
    for zz in range(2):
        sn_flat[pl.ds(zz, 128, stride=2), :] = dens[zz]

    load_plane.wait()
    from_y = product(split(dens[...].reshape(256, 128)), pair(in_plane, 512, 640))
    from_x = product(pair(in_plane, 896, 1024), split(jnp.concatenate([dens[0], dens[1]], axis=1)))
    for zz in range(2):
        grady[zz] = from_y[zz * 128 : zz * 128 + 128]
        gradx[zz] = from_x[:, zz * 128 : zz * 128 + 128]

    for q in range(4):
        twins[q].wait_recv()

        def add_twin(j, carry):
            for u in range(4):
                i = j * 4 + u
                x_lo_, zz, yy = i // 32, lax.rem(i // 4, 8), u
                v = part[i, c] + twin[i]
                for x_hi in range(2):
                    pos = x_hi * 2 + x_lo_
                    qa[pos, yy * 8 + zz] = v[x_hi * 16 : x_hi * 16 + 8]
                    qb[yy, pos * 8 + zz] = v[x_hi * 16 + 8 : x_hi * 16 + 16]
            return carry

        lax.fori_loop(q * 4, q * 4 + 4, add_twin, 0)
    top, low_half = pl.ds(0, 16), pl.ds(16, 16)
    rings = (
        (qa, ra, ha, x_peers, lambda p: at(x_=p), 6),
        (qb, rb, hb, y_peers, lambda p: at(y_=p), 9),
    )
    for own, got, half, (right, across, left), where, k in rings:
        send(own.at[across, top], half.at[0], k, where(right))
        send(own.at[across, low_half], half.at[1], k, where(left))
    pl.semaphore_wait(far, 7)

    def push_density(t, carry):
        pltpu.make_async_remote_copy(
            src_ref=sn.at[t], dst_ref=rn.at[band], send_sem=bulk_s.at[0], recv_sem=bulk_r.at[0],
            device_id={"band": t}, device_id_type=MESH,
        ).start()
        return carry

    lax.fori_loop(band + 1, 128, push_density, 0)
    lax.fori_loop(0, band, push_density, 0)
    rn[band] = sn[band]

    for own, got, half, (right, across, left), where, k in rings:
        send(own.at[right, low_half], got.at[0, low_half], k + 1, where(right))
        send(own.at[left, top], got.at[1, top], k + 1, where(left))

    over_spin.wait_recv()
    along = product(split(dens[s] + far_plane[...]), pair(in_plane, 0, 512))
    turned = product(pair(in_plane, 640, 896), split(jnp.concatenate([along[:, 0:256], along[:, 256:512]], axis=0)))
    sp_flat = sp.reshape(256, 128)
    for half in range(2):
        sp_flat[half * 128 : half * 128 + 128] = turned[:, half * 128 : half * 128 + 128]

    me = s * 128 + band

    def push_spectrum(to, t, carry):
        pltpu.make_async_remote_copy(
            src_ref=sp.at[to * 128 + t], dst_ref=rsp.at[band * 2 + s], send_sem=bulk_s.at[1], recv_sem=bulk_r.at[1],
            device_id={"band": t, "spin": to}, device_id_type=MESH,
        ).start()
        return carry

    for own, got, half, (right, across, left), where, k in rings:
        arrived(half.at[pl.ds(0, 2)], rsem.at[k])
        half[2] = own[right, top] + half[0]
        send(half.at[2], got.at[0, top], k + 1, where(right))
        half[3] = own[left, low_half] + half[1]
        send(half.at[3], got.at[1, low_half], k + 1, where(left))

    for to, start in ((1 - s, band), (s, band + 1)):
        push = functools.partial(push_spectrum, to)
        lax.fori_loop(start, 128, push, 0)
        lax.fori_loop(0, band, push, 0)
    rsp[band * 2 + s] = sp[me]

    arrived(ra, rsem.at[7])
    for t in range(4):
        sub = pl.ds(t * 8, 8)
        a1[t] = qa[x, sub] + (ra[0, sub] + ra[1, sub])
    for d, p in enumerate(y_peers):
        send(a1.at[p], ra2.at[d], 8, at(y_=p))
    arrived(rb, rsem.at[10])
    for t in range(4):
        sub = pl.ds(t * 8, 8)
        b1[t] = qb[y, sub] + (rb[0, sub] + rb[1, sub])
    for d, p in enumerate(x_peers):
        send(b1.at[p], rb2.at[d], 11, at(x_=p))

    load_column.wait()
    all_n = rn.at[pl.ds(0, 127)]
    arrived(all_n, bulk_r.at[0])
    gz.reshape(256, 128)[...] = product(pair(in_column, 512, 768), split(rn.reshape(256, 128)[...]))

    def push_back(t, carry):
        pltpu.make_async_remote_copy(
            src_ref=gz.at[t], dst_ref=rg.at[band], send_sem=bulk_s.at[2], recv_sem=bulk_r.at[2],
            device_id={"band": t}, device_id_type=MESH,
        ).start()
        return carry

    lax.fori_loop(band + 1, 128, push_back, 0)
    lax.fori_loop(0, band, push_back, 0)
    rg[band] = gz[band]

    load_factor.wait()
    lane = lax.broadcasted_iota(jnp.int32, (256, 128), 1)
    row = lax.broadcasted_iota(jnp.int32, (256, 128), 0)
    low = lane < 64
    unit_x, unit_y, unit_z = 2.0 * np.pi / NX, 2.0 * np.pi / NY, 2.0 * np.pi / NZ
    ky = jnp.where(low, lane, lane - 64) - 64 * s
    fy = unit_y * ky.astype(F32)
    fz = unit_z * jnp.where(row >= NZ // 2, row - NZ, row).astype(F32)
    fx = unit_x * jnp.full((1, 128), jnp.where(band >= NX // 2, band - NX, band).astype(F32))
    length_sq = fx * fx + fy * fy + fz * fz
    positive = length_sq > 0
    inverse = jnp.where(positive, 1.0 / jnp.where(positive, length_sq, 1.0), 0.0)
    f0, f1 = factor[0], factor[1]
    first = jnp.where(s == 0, f0, pltpu.roll(f0, 64, 1))
    second = jnp.where(s == 0, pltpu.roll(f1, 64, 1), f1)
    local = 2.0 * jnp.where(low, first, second)

    arrived(ra2, rsem.at[8])
    ab[:, 0] = (a1[y] + ra2[0]) + (ra2[1] + ra2[2])
    arrived(rb2, rsem.at[11])
    ab[:, 1] = (b1[x] + rb2[0]) + (rb2[1] + rb2[2])
    for d, p in enumerate(z_peers):
        send(ab.at[p], rz.at[d], 12, at(z_=p))

    def down(value):
        return jnp.sum(value, axis=0, keepdims=True)

    pairs = ((0, 0), (1, 1), (2, 2), (1, 2), (0, 2), (0, 1))
    arrived(millers.at[pl.ds(0, 7)], rsem.at[5])

    def wave(a, at_z):
        return spacing * (millers[at_z, :, a].astype(F32) + kpoint[a])

    kinetic = [jnp.zeros((1, 128), F32)] * 6
    for at_z in range(8):
        weight = ab[at_z].reshape(16, 128)
        g = [wave(a, at_z) for a in range(3)]
        scaled = [weight * one for one in g]
        kinetic = [t + down(scaled[a] * g[b]) for t, (a, b) in zip(kinetic, pairs)]

    all_sp = rsp.at[pl.ds(0, 255)]
    arrived(all_sp, bulk_r.at[1])
    planes = rsp.reshape(256, 128)[...] * (1.0 / CELLS)
    crossed = pltpu.roll(planes, 64, 1)
    crossed = jnp.where(low, crossed, -crossed)
    spectrum = product(pair(in_column, 0, 512), split(jnp.concatenate([planes, crossed], axis=0)))
    hartree = (4.0 * np.pi) * (spectrum * spectrum) * inverse
    weighting = 2.0 * hartree * inverse + spectrum * local

    sum_h = down(hartree)
    sum_1, sum_z, sum_zz = down(weighting), down(weighting * fz), down(weighting * fz * fz)
    fy1 = fy[0:1]
    spectral = [
        fx * fx * sum_1 - sum_h, fy1 * fy1 * sum_1 - sum_h, sum_zz - sum_h, fy1 * sum_z, fx * sum_z, fx * fy1 * sum_1
    ]

    arrived(rg.at[pl.ds(0, 127)], bulk_r.at[2])
    rg_flat = rg.reshape(256, 128)
    xc = [jnp.zeros((1, 128), F32)] * 6
    for zz in range(2):
        n = dens[zz]
        grads = (gradx[zz], grady[zz], rg_flat[pl.ds(zz, 128, stride=2), :])
        square = grads[0] * grads[0] + grads[1] * grads[1] + grads[2] * grads[2]
        square_held[zz] = square
        room = 4.0 * n * n + 1.0
        kernel = jnp.exp(jnp.log(n) * (-1.0 / 3.0)) * room / (room + square)
        scaled = [kernel * g for g in grads]
        xc = [t + down(scaled[a] * grads[b]) for t, (a, b) in zip(xc, pairs)]

    store_square = pltpu.make_async_copy(square_held, square_out, osem.at[0])
    store_square.start()
    lines = [spectral[a] - kinetic[a] * (1.0 / NPW) - xc[a] * (1.0 / CELLS) for a in range(6)]
    sums = jnp.sum(jnp.concatenate(lines + [jnp.zeros((2, 128), F32)], axis=0), axis=1, keepdims=True)
    diagonal = lax.broadcasted_iota(jnp.int32, (8, 128), 0) == lax.broadcasted_iota(jnp.int32, (8, 128), 1)
    held[0] = down(jnp.where(diagonal, sums, 0.0))

    plane_me = (x * 4 + y) * 2 + c
    stages = ((tot_z, z, [at(z_=p) for p in z_peers], 8), (tot_p, plane_me, plane, 32))
    for stage, (slots, mine, peers, count) in enumerate(stages):
        for peer in peers:
            pltpu.make_async_remote_copy(
                src_ref=held.at[stage], dst_ref=slots.at[mine], send_sem=ssem.at[1], recv_sem=bulk_r.at[3 + stage],
                device_id=peer, device_id_type=MESH,
            ).start()
        slots[mine] = held[stage]
        if stage == 1:
            arrived(rz, rsem.at[12])
            weight = ab[z]
            for d in range(7):
                weight = weight + rz[d]
            weight = weight.reshape(16, 128)
            g = [wave(a, z) for a in range(3)]
            density[...] = 0.5 * (g[0] * g[0] + g[1] * g[1] + g[2] * g[2]) * weight
            store_density = pltpu.make_async_copy(density, density_out, osem.at[1])
            store_density.start()
        arrived(slots.at[pl.ds(0, count - 1)], bulk_r.at[3 + stage])
        held[stage + 1] = down(slots.reshape(count, 128)[...])
    store_totals = pltpu.make_async_copy(held.at[2], totals_out, osem.at[2])
    store_totals.start()

    arrived(coef.at[:, pl.ds(0, 4544)], ssem.at[0])
    arrived(sp.at[pl.ds(0, 38)], ssem.at[1])
    for k, ref in ((0, all_n), (1, all_sp), (2, all_n)):
        arrived(ref, bulk_s.at[k])
    store_square.wait()
    store_density.wait()
    store_totals.wait()


def emit_kernel(totals_any, density_any, square_any, stress_out, density_out, square_out, totals, stress, density, square, sem):
    into = [
        pltpu.make_async_copy(src, dst, sem.at[k])
        for k, (src, dst) in enumerate(((square_any, square), (density_any, density), (totals_any, totals)))
    ]
    for copy in into:
        copy.start()
    out = [
        pltpu.make_async_copy(src, dst, sem.at[3 + k])
        for k, (src, dst) in enumerate(((square, square_out), (density, density_out), (stress, stress_out)))
    ]
    for k in range(2):
        into[k].wait()
        out[k].start()
    into[2].wait()
    for a in range(6):
        stress[a] = totals[0, a]
    out[2].start()
    for copy in out:
        copy.wait()


def shards(coefficients, occupation, miller, density, local_factor):
    pairs = coefficients[0].reshape(2, 2, NPW // 128, 128).transpose(0, 2, 1, 3).reshape(2, NPW // 64, 128)
    in_plane, in_column = [jnp.asarray(t) for t in tables()]
    hbm = pl.BlockSpec(memory_space=pltpu.HBM)
    millers = miller.reshape(3, 16, 128).transpose(1, 0, 2)
    loaded = [((8, 16, 3, 128), jnp.int32), (pairs.shape, BF16), ((2, 128, 128), F32), ((128, 128), F32), ((2, 256, 128), F32)]
    loaded += [(t.shape, BF16) for t in (in_plane, in_column)]
    scratch = loaded + [
        (shape, F32)
        for shape in (
            (128, 2, 128), (128, 2, 128), (128, 2, 128), (128, 2, 128), (256, 1, 128), (256, 1, 128),
            (64, 2, 32, 128), (64, 32, 128), (4, 32, 8, 128), (4, 32, 8, 128), (2, 32, 8, 128), (2, 32, 8, 128),
            (4, 16, 8, 128), (4, 16, 8, 128),
            (4, 8, 8, 128), (4, 8, 8, 128), (3, 8, 8, 128), (3, 8, 8, 128), (8, 2, 8, 128), (7, 2, 8, 128), (2, 128, 128),
            (3, 1, 128), (8, 1, 128), (32, 1, 128), (16, 128), (2, 128, 128),
            (2, 128, 128), (2, 128, 128),
        )
    ]
    dma = pltpu.SemaphoreType.DMA
    results = (
        jax.ShapeDtypeStruct((1, 128), F32),
        jax.ShapeDtypeStruct((16, 128), F32),
        jax.ShapeDtypeStruct((2, 128, 128), F32),
    )
    totals, kinetic_density, square = pl.pallas_call(
        stress_kernel,
        out_shape=results,
        in_specs=[hbm] * 7,
        out_specs=(hbm,) * 3,
        scratch_shapes=[pltpu.SMEM((1, 2), jnp.int32)]
        + [pltpu.VMEM(*one) for one in scratch]
        + [pltpu.SemaphoreType.REGULAR, dma((10,)), dma((3,)), dma((2,)), dma((13,)), dma((3,)), dma((5,))],
        compiler_params=pltpu.CompilerParams(collective_id=0, has_side_effects=True),
    )(occupation, millers, pairs, density[0], local_factor.reshape(2, 256, 128), in_plane, in_column)
    stress, kinetic_density, square = pl.pallas_call(
        emit_kernel,
        out_shape=(jax.ShapeDtypeStruct((6,), F32),) + results[1:],
        in_specs=[hbm] * 3,
        out_specs=(hbm,) * 3,
        scratch_shapes=[
            pltpu.SMEM((1, 128), F32),
            pltpu.SMEM((6,), F32),
            pltpu.VMEM((16, 128), F32),
            pltpu.VMEM((2, 128, 128), F32),
            dma((6,)),
        ],
    )(totals, kinetic_density, square)
    return (stress, kinetic_density.reshape(-1), square[None])


def solution(mesh):
    return jax.shard_map(
        shards,
        mesh=mesh,
        in_specs=(
            P("spin", None, "band", None),
            P("spin", "band"),
            P(None, ("band", "spin")),
            P("spin", "band", None, None),
            P(None, None, "band", None),
        ),
        out_specs=(P(), P(("band", "spin")), P("spin", "band", None, None)),
        check_vma=False,
    )
```

```python
import functools

import jax
import jax.numpy as jnp
import numpy as np
from jax import lax
from jax.experimental import pallas as pl
from jax.experimental.pallas import tpu as pltpu
from jax.sharding import PartitionSpec as P

NPW = 524288
NX = 128
NY = 128
NZ = 256
CELLS = NX * NY * NZ
MESH = pl.DeviceIdType.MESH
F32, BF16 = jnp.float32, jnp.bfloat16

occupation_unit = 1000.0
kpoint = (0.25, 0.125, 0.375)
spacing = 0.25


def derivative_table(length):
    apart = np.arange(length)[:, None] - np.arange(length)[None, :]
    angles = np.pi / length * np.where(apart == 0, 1, apart)
    return np.where(apart == 0, 0.0, 0.5 * (1.0 - 2.0 * (apart % 2)) * np.cos(angles) / np.sin(angles))


def fourier_tables(length):
    index = np.arange(length)
    phases = (index[:, None] * index[None, :]) % length * (2.0 * np.pi / length)
    return np.cos(phases), np.sin(phases)


def halves(table):
    table = np.asarray(table, np.float32)
    high = table.astype(BF16)
    return np.stack([high, (table - high.astype(np.float32)).astype(BF16)])


def tables():
    cos_y, sin_y = fourier_tables(NY)
    cos_x, sin_x = fourier_tables(NX)
    cos_z, sin_z = fourier_tables(NZ)
    lo, hi = slice(0, 64), slice(64, 128)
    re, im = cos_y, -sin_y
    along_y = np.concatenate(
        [re[:, lo], im[:, lo], re[:, hi], im[:, hi], im[:, lo], -re[:, lo], im[:, hi], -re[:, hi], derivative_table(NY).T],
        axis=1,
    )
    along_x = np.concatenate([cos_x, sin_x], axis=1)
    along_z = np.concatenate([cos_z, sin_z], axis=1)
    plane = np.concatenate([along_y, along_x, derivative_table(NX)], axis=1)
    order = np.concatenate([np.arange(0, NZ, 2), np.arange(1, NZ, 2)])
    column = np.concatenate([along_z, derivative_table(NZ)[order][:, order]], axis=1)
    return [halves(t) for t in (plane, column)]


def split(value):
    high = value.astype(BF16)
    return high, (value - high.astype(F32)).astype(BF16)


def product(left, right):
    def dot(a, b):
        return jnp.dot(a, b, preferred_element_type=F32)

    return dot(left[0], right[0]) + (dot(left[0], right[1]) + dot(left[1], right[0]))


def pair(table, first, last):
    return table[0, :, first:last], table[1, :, first:last]


def stress_kernel(
    occ_any, miller_any, coef_any, dens_any, factor_any, plane_any, column_any,
    totals_out, density_out, square_out,
    occ, millers, coef, dens, far_plane, factor, in_plane, in_column,
    sn, rn, gz, rg, sp, rsp,
    part, twin, qa, qb, ra, rb, ha, hb, a1, b1, ra2, rb2, ab, rz, tmp,
    held, tot_z, tot_p, density, square_held,
    far, lsem, osem, ssem, rsem, bulk_s, bulk_r,
):
    band, s = lax.axis_index("band"), lax.axis_index("spin")
    x_lo, z, y, c = band // 64, lax.rem(band // 8, 8), lax.rem(band // 2, 4), lax.rem(band, 2)
    x = s * 2 + x_lo
    other = 1 - c

    def at(x_=None, z_=None, y_=None, c_=None):
        x_ = x if x_ is None else x_
        z_ = z if z_ is None else z_
        y_ = y if y_ is None else y_
        c_ = c if c_ is None else c_
        return {"band": ((lax.rem(x_, 2) * 8 + z_) * 4 + y_) * 2 + c_, "spin": x_ // 2}

    x_peers = [lax.rem(x + d, 4) for d in (1, 2, 3)]
    y_peers = [lax.rem(y + d, 4) for d in (1, 2, 3)]
    z_peers = [lax.rem(z + d, 8) for d in range(1, 8)]
    plane = [
        at(x_=lax.rem(x + d // 8, 4), y_=lax.rem(y + d // 2, 4), c_=lax.rem(c + d, 2)) for d in range(1, 32)
    ]

    def load(src, dst, k):
        copy = pltpu.make_async_copy(src, dst, lsem.at[k])
        copy.start()
        return copy

    load_occ = load(occ_any, occ, 0)
    load_coef = [
        load(coef_any.at[:, pl.ds(q * 2048, 2048)], coef.at[:, pl.ds(q * 2048, 2048)], 1 + q) for q in range(4)
    ]
    barrier = pltpu.get_barrier_semaphore()
    for p in z_peers:
        pl.semaphore_signal(barrier, inc=1, device_id=at(z_=p), device_id_type=MESH)
    for peer in plane:
        pl.semaphore_signal(barrier, inc=1, device_id=peer, device_id_type=MESH)

    load_dens, load_plane, load_column, load_factor, load_miller = [
        load(src, dst, 5 + k)
        for k, (src, dst) in enumerate(
            ((dens_any, dens), (plane_any, in_plane), (column_any, in_column), (factor_any, factor),
             (miller_any, millers.at[z]))
        )
    ]
    def send(src, dst, k, peer):
        copy = pltpu.make_async_remote_copy(
            src_ref=src, dst_ref=dst, send_sem=ssem.at[0], recv_sem=rsem.at[k], device_id=peer, device_id_type=MESH
        )
        copy.start()
        return copy

    def arrived(ref, sem):
        pltpu.make_async_copy(ref, ref, sem).wait()

    load_occ.wait()
    w0 = jnp.full((64, 128), occ[0, 0].astype(F32)) / occupation_unit
    w1 = jnp.full((64, 128), occ[0, 1].astype(F32)) / occupation_unit

    def squares(i, carry):
        for u in range(2):
            rows = pl.ds(pl.multiple_of(i * 256 + u * 128, 128), 128)
            re = coef[0, rows, :].astype(F32)
            im = coef[1, rows, :].astype(F32)
            tmp[u] = re * re + im * im
            both = w0 * tmp[u, pl.ds(0, 64, stride=2), :] + w1 * tmp[u, pl.ds(1, 64, stride=2), :]
            part[i * 2 + u] = both.reshape(2, 32, 128)
        return carry

    for q in range(4):
        load_coef[q].wait()
        lax.fori_loop(q * 8, q * 8 + 8, squares, 0)

    pl.semaphore_wait(barrier, 38)
    twins = [
        send(part.at[pl.ds(q * 16, 16), other], twin.at[pl.ds(q * 16, 16)], q, at(c_=other)) for q in range(4)
    ]
    load_dens.wait()
    over_spin = send(dens.at[1 - s], far_plane, 4, at(x_=x_peers[1]))
    for p in z_peers:
        pl.semaphore_signal(far, inc=1, device_id=at(z_=p), device_id_type=MESH)
    load_miller.wait()
    for p in z_peers:
        send(millers.at[z], millers.at[z], 5, at(z_=p))

    load_plane.wait()
    sn_flat = sn.reshape(512, 128)
    from_x = product(pair(in_plane, 896, 1024), split(jnp.concatenate([dens[0], dens[1]], axis=1)))
    for zz in range(2):
        sn_flat[pl.ds(zz, 128, stride=4), :] = dens[zz]
        sn_flat[pl.ds(2 + zz, 128, stride=4), :] = from_x[:, zz * 128 : zz * 128 + 128]

    for q in range(4):
        twins[q].wait_recv()

        def add_twin(j, carry):
            for u in range(4):
                i = j * 4 + u
                x_lo_, zz, yy = i // 32, lax.rem(i // 4, 8), u
                v = part[i, c] + twin[i]
                for x_hi in range(2):
                    pos = x_hi * 2 + x_lo_
                    qa[pos, yy * 8 + zz] = v[x_hi * 16 : x_hi * 16 + 8]
                    qb[yy, pos * 8 + zz] = v[x_hi * 16 + 8 : x_hi * 16 + 16]
            return carry

        lax.fori_loop(q * 4, q * 4 + 4, add_twin, 0)
    top, low_half = pl.ds(0, 16), pl.ds(16, 16)
    rings = (
        (qa, ra, ha, x_peers, lambda p: at(x_=p), 6),
        (qb, rb, hb, y_peers, lambda p: at(y_=p), 9),
    )
    for own, got, half, (right, across, left), where, k in rings:
        send(own.at[across, top], half.at[0], k, where(right))
        send(own.at[across, low_half], half.at[1], k, where(left))
    pl.semaphore_wait(far, 7)

    def push_density(t, carry):
        pltpu.make_async_remote_copy(
            src_ref=sn.at[t], dst_ref=rn.at[band], send_sem=bulk_s.at[0], recv_sem=bulk_r.at[0],
            device_id={"band": t}, device_id_type=MESH,
        ).start()
        return carry

    lax.fori_loop(band + 1, 128, push_density, 0)
    lax.fori_loop(0, band, push_density, 0)
    rn[band] = sn[band]

    for own, got, half, (right, across, left), where, k in rings:
        send(own.at[right, low_half], got.at[0, low_half], k + 1, where(right))
        send(own.at[left, top], got.at[1, top], k + 1, where(left))

    over_spin.wait_recv()
    along = product(split(dens[s] + far_plane[...]), pair(in_plane, 0, 512))
    turned = product(pair(in_plane, 640, 896), split(jnp.concatenate([along[:, 0:256], along[:, 256:512]], axis=0)))
    sp_flat = sp.reshape(256, 128)
    for half in range(2):
        sp_flat[half * 128 : half * 128 + 128] = turned[:, half * 128 : half * 128 + 128]

    me = s * 128 + band

    def push_spectrum(to, t, carry):
        pltpu.make_async_remote_copy(
            src_ref=sp.at[to * 128 + t], dst_ref=rsp.at[band * 2 + s], send_sem=bulk_s.at[1], recv_sem=bulk_r.at[1],
            device_id={"band": t, "spin": to}, device_id_type=MESH,
        ).start()
        return carry

    for own, got, half, (right, across, left), where, k in rings:
        arrived(half.at[pl.ds(0, 2)], rsem.at[k])
        half[2] = own[right, top] + half[0]
        send(half.at[2], got.at[0, top], k + 1, where(right))
        half[3] = own[left, low_half] + half[1]
        send(half.at[3], got.at[1, low_half], k + 1, where(left))

    for to, start in ((1 - s, band), (s, band + 1)):
        push = functools.partial(push_spectrum, to)
        lax.fori_loop(start, 128, push, 0)
        lax.fori_loop(0, band, push, 0)
    rsp[band * 2 + s] = sp[me]

    arrived(ra, rsem.at[7])
    for t in range(4):
        sub = pl.ds(t * 8, 8)
        a1[t] = qa[x, sub] + (ra[0, sub] + ra[1, sub])
    for d, p in enumerate(y_peers):
        send(a1.at[p], ra2.at[d], 8, at(y_=p))
    arrived(rb, rsem.at[10])
    for t in range(4):
        sub = pl.ds(t * 8, 8)
        b1[t] = qb[y, sub] + (rb[0, sub] + rb[1, sub])
    for d, p in enumerate(x_peers):
        send(b1.at[p], rb2.at[d], 11, at(x_=p))

    load_column.wait()
    all_n = rn.at[pl.ds(0, 127)]
    arrived(all_n, bulk_r.at[0])
    rn_flat = rn.reshape(512, 128)
    n, grad_x = [
        jnp.concatenate([rn_flat[pl.ds(k, 128, stride=4), :], rn_flat[pl.ds(k + 1, 128, stride=4), :]], axis=0)
        for k in (0, 2)
    ]
    halves_n = split(n)
    grads = (grad_x, product(halves_n, pair(in_plane, 512, 640)), product(pair(in_column, 512, 768), halves_n))
    square = grads[0] * grads[0] + grads[1] * grads[1] + grads[2] * grads[2]
    gz_flat = gz.reshape(256, 128)
    for zz in range(2):
        gz_flat[pl.ds(zz, 128, stride=2), :] = square[zz * 128 : zz * 128 + 128]

    def push_back(t, carry):
        pltpu.make_async_remote_copy(
            src_ref=gz.at[t], dst_ref=rg.at[band], send_sem=bulk_s.at[2], recv_sem=bulk_r.at[2],
            device_id={"band": t}, device_id_type=MESH,
        ).start()
        return carry

    lax.fori_loop(band + 1, 128, push_back, 0)
    lax.fori_loop(0, band, push_back, 0)
    rg[band] = gz[band]

    def down(value):
        return jnp.sum(value, axis=0, keepdims=True)

    pairs = ((0, 0), (1, 1), (2, 2), (1, 2), (0, 2), (0, 1))
    room = 4.0 * n * n + 1.0
    kernel = jnp.exp(jnp.log(n) * (-1.0 / 3.0)) * room / (room + square)
    scaled_grads = [kernel * g for g in grads]
    xc = [down(scaled_grads[a] * grads[b]) for a, b in pairs]

    load_factor.wait()
    lane = lax.broadcasted_iota(jnp.int32, (256, 128), 1)
    row = lax.broadcasted_iota(jnp.int32, (256, 128), 0)
    low = lane < 64
    unit_x, unit_y, unit_z = 2.0 * np.pi / NX, 2.0 * np.pi / NY, 2.0 * np.pi / NZ
    ky = jnp.where(low, lane, lane - 64) - 64 * s
    fy = unit_y * ky.astype(F32)
    fz = unit_z * jnp.where(row >= NZ // 2, row - NZ, row).astype(F32)
    fx = unit_x * jnp.full((1, 128), jnp.where(band >= NX // 2, band - NX, band).astype(F32))
    length_sq = fx * fx + fy * fy + fz * fz
    positive = length_sq > 0
    inverse = jnp.where(positive, 1.0 / jnp.where(positive, length_sq, 1.0), 0.0)
    f0, f1 = factor[0], factor[1]
    first = jnp.where(s == 0, f0, pltpu.roll(f0, 64, 1))
    second = jnp.where(s == 0, pltpu.roll(f1, 64, 1), f1)
    local = 2.0 * jnp.where(low, first, second)

    arrived(ra2, rsem.at[8])
    ab[:, 0] = (a1[y] + ra2[0]) + (ra2[1] + ra2[2])
    arrived(rb2, rsem.at[11])
    ab[:, 1] = (b1[x] + rb2[0]) + (rb2[1] + rb2[2])
    for d, p in enumerate(z_peers):
        send(ab.at[p], rz.at[d], 12, at(z_=p))

    arrived(millers.at[pl.ds(0, 7)], rsem.at[5])

    def wave(a, at_z):
        return spacing * (millers[at_z, :, a].astype(F32) + kpoint[a])

    kinetic = [jnp.zeros((1, 128), F32)] * 6
    for at_z in range(8):
        weight = ab[at_z].reshape(16, 128)
        g = [wave(a, at_z) for a in range(3)]
        scaled = [weight * one for one in g]
        kinetic = [t + down(scaled[a] * g[b]) for t, (a, b) in zip(kinetic, pairs)]

    all_sp = rsp.at[pl.ds(0, 255)]
    arrived(all_sp, bulk_r.at[1])
    planes = rsp.reshape(256, 128)[...] * (1.0 / CELLS)
    crossed = pltpu.roll(planes, 64, 1)
    crossed = jnp.where(low, crossed, -crossed)
    spectrum = product(pair(in_column, 0, 512), split(jnp.concatenate([planes, crossed], axis=0)))
    hartree = (4.0 * np.pi) * (spectrum * spectrum) * inverse
    weighting = 2.0 * hartree * inverse + spectrum * local

    sum_h = down(hartree)
    sum_1, sum_z, sum_zz = down(weighting), down(weighting * fz), down(weighting * fz * fz)
    fy1 = fy[0:1]
    spectral = [
        fx * fx * sum_1 - sum_h, fy1 * fy1 * sum_1 - sum_h, sum_zz - sum_h, fy1 * sum_z, fx * sum_z, fx * fy1 * sum_1
    ]

    lines = [spectral[a] - kinetic[a] * (1.0 / NPW) - xc[a] * (1.0 / CELLS) for a in range(6)]
    sums = jnp.sum(jnp.concatenate(lines + [jnp.zeros((2, 128), F32)], axis=0), axis=1, keepdims=True)
    diagonal = lax.broadcasted_iota(jnp.int32, (8, 128), 0) == lax.broadcasted_iota(jnp.int32, (8, 128), 1)
    held[0] = down(jnp.where(diagonal, sums, 0.0))

    plane_me = (x * 4 + y) * 2 + c
    stages = ((tot_z, z, [at(z_=p) for p in z_peers], 8), (tot_p, plane_me, plane, 32))
    for stage, (slots, mine, peers, count) in enumerate(stages):
        for peer in peers:
            pltpu.make_async_remote_copy(
                src_ref=held.at[stage], dst_ref=slots.at[mine], send_sem=ssem.at[1], recv_sem=bulk_r.at[3 + stage],
                device_id=peer, device_id_type=MESH,
            ).start()
        slots[mine] = held[stage]
        if stage == 1:
            arrived(rz, rsem.at[12])
            weight = ab[z]
            for d in range(7):
                weight = weight + rz[d]
            weight = weight.reshape(16, 128)
            g = [wave(a, z) for a in range(3)]
            density[...] = 0.5 * (g[0] * g[0] + g[1] * g[1] + g[2] * g[2]) * weight
            store_density = pltpu.make_async_copy(density, density_out, osem.at[1])
            store_density.start()
            arrived(rg.at[pl.ds(0, 127)], bulk_r.at[2])
            rg_flat = rg.reshape(256, 128)
            for zz in range(2):
                square_held[zz] = rg_flat[pl.ds(zz, 128, stride=2), :]
            store_square = pltpu.make_async_copy(square_held, square_out, osem.at[0])
            store_square.start()
        arrived(slots.at[pl.ds(0, count - 1)], bulk_r.at[3 + stage])
        held[stage + 1] = down(slots.reshape(count, 128)[...])
    store_totals = pltpu.make_async_copy(held.at[2], totals_out, osem.at[2])
    store_totals.start()

    arrived(coef.at[:, pl.ds(0, 4544)], ssem.at[0])
    arrived(sp.at[pl.ds(0, 38)], ssem.at[1])
    for k, ref in ((0, all_n), (1, all_sp), (2, rg.at[pl.ds(0, 127)])):
        arrived(ref, bulk_s.at[k])
    store_square.wait()
    store_density.wait()
    store_totals.wait()


def emit_kernel(totals_any, density_any, square_any, stress_out, density_out, square_out, totals, stress, density, square, sem):
    into = [
        pltpu.make_async_copy(src, dst, sem.at[k])
        for k, (src, dst) in enumerate(((square_any, square), (density_any, density), (totals_any, totals)))
    ]
    for copy in into:
        copy.start()
    out = [
        pltpu.make_async_copy(src, dst, sem.at[3 + k])
        for k, (src, dst) in enumerate(((square, square_out), (density, density_out), (stress, stress_out)))
    ]
    for k in range(2):
        into[k].wait()
        out[k].start()
    into[2].wait()
    for a in range(6):
        stress[a] = totals[0, a]
    out[2].start()
    for copy in out:
        copy.wait()


def shards(coefficients, occupation, miller, density, local_factor):
    pairs = coefficients[0].reshape(2, 2, NPW // 128, 128).transpose(0, 2, 1, 3).reshape(2, NPW // 64, 128)
    in_plane, in_column = [jnp.asarray(t) for t in tables()]
    hbm = pl.BlockSpec(memory_space=pltpu.HBM)
    millers = miller.reshape(3, 16, 128).transpose(1, 0, 2)
    loaded = [((8, 16, 3, 128), jnp.int32), (pairs.shape, BF16), ((2, 128, 128), F32), ((128, 128), F32), ((2, 256, 128), F32)]
    loaded += [(t.shape, BF16) for t in (in_plane, in_column)]
    scratch = loaded + [
        (shape, F32)
        for shape in (
            (128, 4, 128), (128, 4, 128), (128, 2, 128), (128, 2, 128), (256, 1, 128), (256, 1, 128),
            (64, 2, 32, 128), (64, 32, 128), (4, 32, 8, 128), (4, 32, 8, 128), (2, 32, 8, 128), (2, 32, 8, 128),
            (4, 16, 8, 128), (4, 16, 8, 128),
            (4, 8, 8, 128), (4, 8, 8, 128), (3, 8, 8, 128), (3, 8, 8, 128), (8, 2, 8, 128), (7, 2, 8, 128), (2, 128, 128),
            (3, 1, 128), (8, 1, 128), (32, 1, 128), (16, 128), (2, 128, 128),
        )
    ]
    dma = pltpu.SemaphoreType.DMA
    results = (
        jax.ShapeDtypeStruct((1, 128), F32),
        jax.ShapeDtypeStruct((16, 128), F32),
        jax.ShapeDtypeStruct((2, 128, 128), F32),
    )
    totals, kinetic_density, square = pl.pallas_call(
        stress_kernel,
        out_shape=results,
        in_specs=[hbm] * 7,
        out_specs=(hbm,) * 3,
        scratch_shapes=[pltpu.SMEM((1, 2), jnp.int32)]
        + [pltpu.VMEM(*one) for one in scratch]
        + [pltpu.SemaphoreType.REGULAR, dma((10,)), dma((3,)), dma((2,)), dma((13,)), dma((3,)), dma((5,))],
        compiler_params=pltpu.CompilerParams(collective_id=0, has_side_effects=True),
    )(occupation, millers, pairs, density[0], local_factor.reshape(2, 256, 128), in_plane, in_column)
    stress, kinetic_density, square = pl.pallas_call(
        emit_kernel,
        out_shape=(jax.ShapeDtypeStruct((6,), F32),) + results[1:],
        in_specs=[hbm] * 3,
        out_specs=(hbm,) * 3,
        scratch_shapes=[
            pltpu.SMEM((1, 128), F32),
            pltpu.SMEM((6,), F32),
            pltpu.VMEM((16, 128), F32),
            pltpu.VMEM((2, 128, 128), F32),
            dma((6,)),
        ],
    )(totals, kinetic_density, square)
    return (stress, kinetic_density.reshape(-1), square[None])


def solution(mesh):
    return jax.shard_map(
        shards,
        mesh=mesh,
        in_specs=(
            P("spin", None, "band", None),
            P("spin", "band"),
            P(None, ("band", "spin")),
            P("spin", "band", None, None),
            P(None, None, "band", None),
        ),
        out_specs=(P(), P(("band", "spin")), P("spin", "band", None, None)),
        check_vma=False,
    )
```

```python
import functools

import jax
import jax.numpy as jnp
import numpy as np
from jax import lax
from jax.experimental import pallas as pl
from jax.experimental.pallas import tpu as pltpu
from jax.sharding import PartitionSpec as P

NPW = 524288
NX = 128
NY = 128
NZ = 256
CELLS = NX * NY * NZ
MESH = pl.DeviceIdType.MESH
F32, BF16 = jnp.float32, jnp.bfloat16

occupation_unit = 1000.0
kpoint = (0.25, 0.125, 0.375)
spacing = 0.25


def derivative_table(length):
    apart = np.arange(length)[:, None] - np.arange(length)[None, :]
    angles = np.pi / length * np.where(apart == 0, 1, apart)
    return np.where(apart == 0, 0.0, 0.5 * (1.0 - 2.0 * (apart % 2)) * np.cos(angles) / np.sin(angles))


def fourier_tables(length):
    index = np.arange(length)
    phases = (index[:, None] * index[None, :]) % length * (2.0 * np.pi / length)
    return np.cos(phases), np.sin(phases)


def halves(table):
    table = np.asarray(table, np.float32)
    high = table.astype(BF16)
    return np.stack([high, (table - high.astype(np.float32)).astype(BF16)])


def tables():
    cos_y, sin_y = fourier_tables(NY)
    cos_x, sin_x = fourier_tables(NX)
    cos_z, sin_z = fourier_tables(NZ)
    lo, hi = slice(0, 64), slice(64, 128)
    re, im = cos_y, -sin_y
    along_y = np.concatenate(
        [re[:, lo], im[:, lo], re[:, hi], im[:, hi], im[:, lo], -re[:, lo], im[:, hi], -re[:, hi], derivative_table(NY).T],
        axis=1,
    )
    along_x = np.concatenate([cos_x, sin_x], axis=1)
    along_z = np.concatenate([cos_z, sin_z], axis=1)
    plane = np.concatenate([along_y, along_x, derivative_table(NX)], axis=1)
    order = np.concatenate([np.arange(0, NZ, 2), np.arange(1, NZ, 2)])
    column = np.concatenate([along_z, derivative_table(NZ)[order][:, order]], axis=1)
    return [halves(t) for t in (plane, column)]


def split(value):
    high = value.astype(BF16)
    return high, (value - high.astype(F32)).astype(BF16)


def product(left, right):
    def dot(a, b):
        return jnp.dot(a, b, preferred_element_type=F32)

    return dot(left[0], right[0]) + (dot(left[0], right[1]) + dot(left[1], right[0]))


def pair(table, first, last):
    return table[0, :, first:last], table[1, :, first:last]


def stress_kernel(
    occ_any, miller_any, coef_any, dens_any, factor_any, plane_any, column_any,
    totals_out, density_out, square_out,
    occ, millers, coef, dens, far_plane, factor, in_plane, in_column,
    sn, rn, gz, rg, sp, rsp,
    part, twin, qa, qb, ra, rb, ha, hb, a1, b1, ra2, rb2, ab, rz, tmp,
    held, tot_z, tot_p, density, square_held,
    far, lsem, osem, ssem, rsem, bulk_s, bulk_r,
):
    band, s = lax.axis_index("band"), lax.axis_index("spin")
    x_lo, z, y, c = band // 64, lax.rem(band // 8, 8), lax.rem(band // 2, 4), lax.rem(band, 2)
    x = s * 2 + x_lo
    other = 1 - c

    def at(x_=None, z_=None, y_=None, c_=None):
        x_ = x if x_ is None else x_
        z_ = z if z_ is None else z_
        y_ = y if y_ is None else y_
        c_ = c if c_ is None else c_
        return {"band": ((lax.rem(x_, 2) * 8 + z_) * 4 + y_) * 2 + c_, "spin": x_ // 2}

    x_peers = [lax.rem(x + d, 4) for d in (1, 2, 3)]
    y_peers = [lax.rem(y + d, 4) for d in (1, 2, 3)]
    z_peers = [lax.rem(z + d, 8) for d in range(1, 8)]
    plane = [
        at(x_=lax.rem(x + d // 8, 4), y_=lax.rem(y + d // 2, 4), c_=lax.rem(c + d, 2)) for d in range(1, 32)
    ]

    def load(src, dst, k):
        copy = pltpu.make_async_copy(src, dst, lsem.at[k])
        copy.start()
        return copy

    load_occ = load(occ_any, occ, 0)
    load_coef = [
        load(coef_any.at[:, pl.ds(q * 2048, 2048)], coef.at[:, pl.ds(q * 2048, 2048)], 1 + q) for q in range(4)
    ]
    barrier = pltpu.get_barrier_semaphore()
    for p in z_peers:
        pl.semaphore_signal(barrier, inc=1, device_id=at(z_=p), device_id_type=MESH)
    for peer in plane:
        pl.semaphore_signal(barrier, inc=1, device_id=peer, device_id_type=MESH)

    load_dens, load_plane, load_column, load_factor, load_miller = [
        load(src, dst, 5 + k)
        for k, (src, dst) in enumerate(
            ((dens_any, dens), (plane_any, in_plane), (column_any, in_column), (factor_any, factor),
             (miller_any, millers.at[z]))
        )
    ]
    def send(src, dst, k, peer):
        copy = pltpu.make_async_remote_copy(
            src_ref=src, dst_ref=dst, send_sem=ssem.at[0], recv_sem=rsem.at[k], device_id=peer, device_id_type=MESH
        )
        copy.start()
        return copy

    def arrived(ref, sem):
        pltpu.make_async_copy(ref, ref, sem).wait()

    load_occ.wait()
    w0 = jnp.full((64, 128), occ[0, 0].astype(F32)) / occupation_unit
    w1 = jnp.full((64, 128), occ[0, 1].astype(F32)) / occupation_unit

    def squares(i, carry):
        for u in range(2):
            rows = pl.ds(pl.multiple_of(i * 256 + u * 128, 128), 128)
            re = coef[0, rows, :].astype(F32)
            im = coef[1, rows, :].astype(F32)
            tmp[u] = re * re + im * im
            both = w0 * tmp[u, pl.ds(0, 64, stride=2), :] + w1 * tmp[u, pl.ds(1, 64, stride=2), :]
            part[i * 2 + u] = both.reshape(2, 32, 128)
        return carry

    for q in range(4):
        load_coef[q].wait()
        lax.fori_loop(q * 8, q * 8 + 8, squares, 0)

    pl.semaphore_wait(barrier, 38)
    twins = [
        send(part.at[pl.ds(q * 16, 16), other], twin.at[pl.ds(q * 16, 16)], q, at(c_=other)) for q in range(4)
    ]
    load_dens.wait()
    over_spin = send(dens.at[1 - s], far_plane, 4, at(x_=x_peers[1]))
    for p in z_peers:
        pl.semaphore_signal(far, inc=1, device_id=at(z_=p), device_id_type=MESH)
    load_miller.wait()
    for p in z_peers:
        send(millers.at[z], millers.at[z], 5, at(z_=p))

    load_plane.wait()
    sn_flat = sn.reshape(512, 128)
    from_x = product(pair(in_plane, 896, 1024), split(jnp.concatenate([dens[0], dens[1]], axis=1)))
    for zz in range(2):
        sn_flat[pl.ds(zz, 128, stride=4), :] = dens[zz]
        sn_flat[pl.ds(2 + zz, 128, stride=4), :] = from_x[:, zz * 128 : zz * 128 + 128]

    for q in range(4):
        twins[q].wait_recv()

        def add_twin(j, carry):
            for u in range(4):
                i = j * 4 + u
                x_lo_, zz, yy = i // 32, lax.rem(i // 4, 8), u
                v = part[i, c] + twin[i]
                for x_hi in range(2):
                    pos = x_hi * 2 + x_lo_
                    qa[pos, yy * 8 + zz] = v[x_hi * 16 : x_hi * 16 + 8]
                    qb[yy, pos * 8 + zz] = v[x_hi * 16 + 8 : x_hi * 16 + 16]
            return carry

        lax.fori_loop(q * 4, q * 4 + 4, add_twin, 0)
    top, low_half = pl.ds(0, 16), pl.ds(16, 16)
    rings = (
        (qa, ra, ha, x_peers, lambda p: at(x_=p), 6),
        (qb, rb, hb, y_peers, lambda p: at(y_=p), 9),
    )
    for own, got, half, (right, across, left), where, k in rings:
        send(own.at[across, top], half.at[0], k, where(right))
        send(own.at[across, low_half], half.at[1], k, where(left))
    pl.semaphore_wait(far, 7)

    def push_density(t, carry):
        pltpu.make_async_remote_copy(
            src_ref=sn.at[t], dst_ref=rn.at[band], send_sem=bulk_s.at[0], recv_sem=bulk_r.at[0],
            device_id={"band": t}, device_id_type=MESH,
        ).start()
        return carry

    lax.fori_loop(band + 1, 128, push_density, 0)
    lax.fori_loop(0, band, push_density, 0)
    rn[band] = sn[band]

    for own, got, half, (right, across, left), where, k in rings:
        send(own.at[right, low_half], got.at[0, low_half], k + 1, where(right))
        send(own.at[left, top], got.at[1, top], k + 1, where(left))

    over_spin.wait_recv()
    along = product(split(dens[s] + far_plane[...]), pair(in_plane, 0, 512))
    turned = product(pair(in_plane, 640, 896), split(jnp.concatenate([along[:, 0:256], along[:, 256:512]], axis=0)))
    sp_flat = sp.reshape(256, 128)
    for half in range(2):
        sp_flat[half * 128 : half * 128 + 128] = turned[:, half * 128 : half * 128 + 128]

    me = s * 128 + band

    def push_spectrum(to, t, carry):
        pltpu.make_async_remote_copy(
            src_ref=sp.at[to * 128 + t], dst_ref=rsp.at[band * 2 + s], send_sem=bulk_s.at[1], recv_sem=bulk_r.at[1],
            device_id={"band": t, "spin": to}, device_id_type=MESH,
        ).start()
        return carry

    for own, got, half, (right, across, left), where, k in rings:
        arrived(half.at[pl.ds(0, 2)], rsem.at[k])
        half[2] = own[right, top] + half[0]
        send(half.at[2], got.at[0, top], k + 1, where(right))
        half[3] = own[left, low_half] + half[1]
        send(half.at[3], got.at[1, low_half], k + 1, where(left))

    for to, start in ((1 - s, band), (s, band + 1)):
        push = functools.partial(push_spectrum, to)
        lax.fori_loop(start, 128, push, 0)
        lax.fori_loop(0, band, push, 0)
    rsp[band * 2 + s] = sp[me]

    arrived(ra, rsem.at[7])
    for t in range(4):
        sub = pl.ds(t * 8, 8)
        a1[t] = qa[x, sub] + (ra[0, sub] + ra[1, sub])
    for d, p in enumerate(y_peers):
        send(a1.at[p], ra2.at[d], 8, at(y_=p))
    arrived(rb, rsem.at[10])
    for t in range(4):
        sub = pl.ds(t * 8, 8)
        b1[t] = qb[y, sub] + (rb[0, sub] + rb[1, sub])
    for d, p in enumerate(x_peers):
        send(b1.at[p], rb2.at[d], 11, at(x_=p))

    load_column.wait()
    all_n = rn.at[pl.ds(0, 127)]
    arrived(all_n, bulk_r.at[0])
    rn_flat = rn.reshape(512, 128)
    n, grad_x = [
        jnp.concatenate([rn_flat[pl.ds(k, 128, stride=4), :], rn_flat[pl.ds(k + 1, 128, stride=4), :]], axis=0)
        for k in (0, 2)
    ]
    halves_n = split(n)
    grads = (grad_x, product(halves_n, pair(in_plane, 512, 640)), product(pair(in_column, 512, 768), halves_n))
    square = grads[0] * grads[0] + grads[1] * grads[1] + grads[2] * grads[2]
    gz_flat = gz.reshape(256, 128)
    for zz in range(2):
        gz_flat[pl.ds(zz, 128, stride=2), :] = square[zz * 128 : zz * 128 + 128]

    def down(value):
        return jnp.sum(value, axis=0, keepdims=True)

    pairs = ((0, 0), (1, 1), (2, 2), (1, 2), (0, 2), (0, 1))
    room = 4.0 * n * n + 1.0
    kernel = jnp.exp(jnp.log(n) * (-1.0 / 3.0)) * room / (room + square)
    scaled_grads = [kernel * g for g in grads]
    xc = [down(scaled_grads[a] * grads[b]) for a, b in pairs]

    load_factor.wait()
    lane = lax.broadcasted_iota(jnp.int32, (256, 128), 1)
    row = lax.broadcasted_iota(jnp.int32, (256, 128), 0)
    low = lane < 64
    unit_x, unit_y, unit_z = 2.0 * np.pi / NX, 2.0 * np.pi / NY, 2.0 * np.pi / NZ
    ky = jnp.where(low, lane, lane - 64) - 64 * s
    fy = unit_y * ky.astype(F32)
    fz = unit_z * jnp.where(row >= NZ // 2, row - NZ, row).astype(F32)
    fx = unit_x * jnp.full((1, 128), jnp.where(band >= NX // 2, band - NX, band).astype(F32))
    length_sq = fx * fx + fy * fy + fz * fz
    positive = length_sq > 0
    inverse = jnp.where(positive, 1.0 / jnp.where(positive, length_sq, 1.0), 0.0)
    f0, f1 = factor[0], factor[1]
    first = jnp.where(s == 0, f0, pltpu.roll(f0, 64, 1))
    second = jnp.where(s == 0, pltpu.roll(f1, 64, 1), f1)
    local = 2.0 * jnp.where(low, first, second)

    arrived(ra2, rsem.at[8])
    ab[:, 0] = (a1[y] + ra2[0]) + (ra2[1] + ra2[2])
    arrived(rb2, rsem.at[11])
    ab[:, 1] = (b1[x] + rb2[0]) + (rb2[1] + rb2[2])
    for d, p in enumerate(z_peers):
        send(ab.at[p], rz.at[d], 12, at(z_=p))

    arrived(millers.at[pl.ds(0, 7)], rsem.at[5])

    def wave(a, at_z):
        return spacing * (millers[at_z, :, a].astype(F32) + kpoint[a])

    kinetic = [jnp.zeros((1, 128), F32)] * 6
    for at_z in range(8):
        weight = ab[at_z].reshape(16, 128)
        g = [wave(a, at_z) for a in range(3)]
        scaled = [weight * one for one in g]
        kinetic = [t + down(scaled[a] * g[b]) for t, (a, b) in zip(kinetic, pairs)]

    all_sp = rsp.at[pl.ds(0, 255)]
    arrived(all_sp, bulk_r.at[1])
    planes = rsp.reshape(256, 128)[...] * (1.0 / CELLS)
    crossed = pltpu.roll(planes, 64, 1)
    crossed = jnp.where(low, crossed, -crossed)
    spectrum = product(pair(in_column, 0, 512), split(jnp.concatenate([planes, crossed], axis=0)))
    hartree = (4.0 * np.pi) * (spectrum * spectrum) * inverse
    weighting = 2.0 * hartree * inverse + spectrum * local

    sum_h = down(hartree)
    sum_1, sum_z, sum_zz = down(weighting), down(weighting * fz), down(weighting * fz * fz)
    fy1 = fy[0:1]
    spectral = [
        fx * fx * sum_1 - sum_h, fy1 * fy1 * sum_1 - sum_h, sum_zz - sum_h, fy1 * sum_z, fx * sum_z, fx * fy1 * sum_1
    ]

    lines = [spectral[a] - kinetic[a] * (1.0 / NPW) - xc[a] * (1.0 / CELLS) for a in range(6)]
    sums = jnp.sum(jnp.concatenate(lines + [jnp.zeros((2, 128), F32)], axis=0), axis=1, keepdims=True)
    diagonal = lax.broadcasted_iota(jnp.int32, (8, 128), 0) == lax.broadcasted_iota(jnp.int32, (8, 128), 1)
    held[0] = down(jnp.where(diagonal, sums, 0.0))

    def push_back(t, carry):
        pltpu.make_async_remote_copy(
            src_ref=gz.at[t], dst_ref=rg.at[band], send_sem=bulk_s.at[2], recv_sem=bulk_r.at[2],
            device_id={"band": t}, device_id_type=MESH,
        ).start()
        return carry

    plane_me = (x * 4 + y) * 2 + c
    stages = ((tot_z, z, [at(z_=p) for p in z_peers], 8), (tot_p, plane_me, plane, 32))
    for stage, (slots, mine, peers, count) in enumerate(stages):
        for peer in peers:
            pltpu.make_async_remote_copy(
                src_ref=held.at[stage], dst_ref=slots.at[mine], send_sem=ssem.at[1], recv_sem=bulk_r.at[3 + stage],
                device_id=peer, device_id_type=MESH,
            ).start()
        slots[mine] = held[stage]
        if stage == 0:
            lax.fori_loop(band + 1, 128, push_back, 0)
            lax.fori_loop(0, band, push_back, 0)
            rg[band] = gz[band]
        if stage == 1:
            arrived(rz, rsem.at[12])
            weight = ab[z]
            for d in range(7):
                weight = weight + rz[d]
            weight = weight.reshape(16, 128)
            g = [wave(a, z) for a in range(3)]
            density[...] = 0.5 * (g[0] * g[0] + g[1] * g[1] + g[2] * g[2]) * weight
            store_density = pltpu.make_async_copy(density, density_out, osem.at[1])
            store_density.start()
        arrived(slots.at[pl.ds(0, count - 1)], bulk_r.at[3 + stage])
        held[stage + 1] = down(slots.reshape(count, 128)[...])
    store_totals = pltpu.make_async_copy(held.at[2], totals_out, osem.at[2])
    store_totals.start()
    arrived(rg.at[pl.ds(0, 127)], bulk_r.at[2])
    rg_flat = rg.reshape(256, 128)
    for zz in range(2):
        square_held[zz] = rg_flat[pl.ds(zz, 128, stride=2), :]
    store_square = pltpu.make_async_copy(square_held, square_out, osem.at[0])
    store_square.start()

    arrived(coef.at[:, pl.ds(0, 4544)], ssem.at[0])
    arrived(sp.at[pl.ds(0, 38)], ssem.at[1])
    for k, ref in ((0, all_n), (1, all_sp), (2, rg.at[pl.ds(0, 127)])):
        arrived(ref, bulk_s.at[k])
    store_square.wait()
    store_density.wait()
    store_totals.wait()


def emit_kernel(totals_any, density_any, square_any, stress_out, density_out, square_out, totals, stress, density, square, sem):
    into = [
        pltpu.make_async_copy(src, dst, sem.at[k])
        for k, (src, dst) in enumerate(((square_any, square), (density_any, density), (totals_any, totals)))
    ]
    for copy in into:
        copy.start()
    out = [
        pltpu.make_async_copy(src, dst, sem.at[3 + k])
        for k, (src, dst) in enumerate(((square, square_out), (density, density_out), (stress, stress_out)))
    ]
    for k in range(2):
        into[k].wait()
        out[k].start()
    into[2].wait()
    for a in range(6):
        stress[a] = totals[0, a]
    out[2].start()
    for copy in out:
        copy.wait()


def shards(coefficients, occupation, miller, density, local_factor):
    pairs = coefficients[0].reshape(2, 2, NPW // 128, 128).transpose(0, 2, 1, 3).reshape(2, NPW // 64, 128)
    in_plane, in_column = [jnp.asarray(t) for t in tables()]
    hbm = pl.BlockSpec(memory_space=pltpu.HBM)
    millers = miller.reshape(3, 16, 128).transpose(1, 0, 2)
    loaded = [((8, 16, 3, 128), jnp.int32), (pairs.shape, BF16), ((2, 128, 128), F32), ((128, 128), F32), ((2, 256, 128), F32)]
    loaded += [(t.shape, BF16) for t in (in_plane, in_column)]
    scratch = loaded + [
        (shape, F32)
        for shape in (
            (128, 4, 128), (128, 4, 128), (128, 2, 128), (128, 2, 128), (256, 1, 128), (256, 1, 128),
            (64, 2, 32, 128), (64, 32, 128), (4, 32, 8, 128), (4, 32, 8, 128), (2, 32, 8, 128), (2, 32, 8, 128),
            (4, 16, 8, 128), (4, 16, 8, 128),
            (4, 8, 8, 128), (4, 8, 8, 128), (3, 8, 8, 128), (3, 8, 8, 128), (8, 2, 8, 128), (7, 2, 8, 128), (2, 128, 128),
            (3, 1, 128), (8, 1, 128), (32, 1, 128), (16, 128), (2, 128, 128),
        )
    ]
    dma = pltpu.SemaphoreType.DMA
    results = (
        jax.ShapeDtypeStruct((1, 128), F32),
        jax.ShapeDtypeStruct((16, 128), F32),
        jax.ShapeDtypeStruct((2, 128, 128), F32),
    )
    totals, kinetic_density, square = pl.pallas_call(
        stress_kernel,
        out_shape=results,
        in_specs=[hbm] * 7,
        out_specs=(hbm,) * 3,
        scratch_shapes=[pltpu.SMEM((1, 2), jnp.int32)]
        + [pltpu.VMEM(*one) for one in scratch]
        + [pltpu.SemaphoreType.REGULAR, dma((10,)), dma((3,)), dma((2,)), dma((13,)), dma((3,)), dma((5,))],
        compiler_params=pltpu.CompilerParams(collective_id=0, has_side_effects=True),
    )(occupation, millers, pairs, density[0], local_factor.reshape(2, 256, 128), in_plane, in_column)
    stress, kinetic_density, square = pl.pallas_call(
        emit_kernel,
        out_shape=(jax.ShapeDtypeStruct((6,), F32),) + results[1:],
        in_specs=[hbm] * 3,
        out_specs=(hbm,) * 3,
        scratch_shapes=[
            pltpu.SMEM((1, 128), F32),
            pltpu.SMEM((6,), F32),
            pltpu.VMEM((16, 128), F32),
            pltpu.VMEM((2, 128, 128), F32),
            dma((6,)),
        ],
    )(totals, kinetic_density, square)
    return (stress, kinetic_density.reshape(-1), square[None])


def solution(mesh):
    return jax.shard_map(
        shards,
        mesh=mesh,
        in_specs=(
            P("spin", None, "band", None),
            P("spin", "band"),
            P(None, ("band", "spin")),
            P("spin", "band", None, None),
            P(None, None, "band", None),
        ),
        out_specs=(P(), P(("band", "spin")), P("spin", "band", None, None)),
        check_vma=False,
    )
```

```python
import functools

import jax
import jax.numpy as jnp
import numpy as np
from jax import lax
from jax.experimental import pallas as pl
from jax.experimental.pallas import tpu as pltpu
from jax.sharding import PartitionSpec as P

NPW = 524288
NX = 128
NY = 128
NZ = 256
CELLS = NX * NY * NZ
MESH = pl.DeviceIdType.MESH
F32, BF16 = jnp.float32, jnp.bfloat16

occupation_unit = 1000.0
kpoint = (0.25, 0.125, 0.375)
spacing = 0.25


def derivative_table(length):
    apart = np.arange(length)[:, None] - np.arange(length)[None, :]
    angles = np.pi / length * np.where(apart == 0, 1, apart)
    return np.where(apart == 0, 0.0, 0.5 * (1.0 - 2.0 * (apart % 2)) * np.cos(angles) / np.sin(angles))


def fourier_tables(length):
    index = np.arange(length)
    phases = (index[:, None] * index[None, :]) % length * (2.0 * np.pi / length)
    return np.cos(phases), np.sin(phases)


def halves(table):
    table = np.asarray(table, np.float32)
    high = table.astype(BF16)
    return np.stack([high, (table - high.astype(np.float32)).astype(BF16)])


def tables():
    cos_y, sin_y = fourier_tables(NY)
    cos_x, sin_x = fourier_tables(NX)
    cos_z, sin_z = fourier_tables(NZ)
    lo, hi = slice(0, 64), slice(64, 128)
    re, im = cos_y, -sin_y
    along_y = np.concatenate(
        [re[:, lo], im[:, lo], re[:, hi], im[:, hi], im[:, lo], -re[:, lo], im[:, hi], -re[:, hi], derivative_table(NY).T],
        axis=1,
    )
    along_x = np.concatenate([cos_x, sin_x], axis=1)
    along_z = np.concatenate([cos_z, sin_z], axis=1)
    plane = np.concatenate([along_y, along_x, derivative_table(NX)], axis=1)
    order = np.concatenate([np.arange(0, NZ, 2), np.arange(1, NZ, 2)])
    column = np.concatenate([along_z, derivative_table(NZ)[order][:, order]], axis=1)
    return [halves(t) for t in (plane, column)]


def split(value):
    high = value.astype(BF16)
    return high, (value - high.astype(F32)).astype(BF16)


def product(left, right):
    def dot(a, b):
        return jnp.dot(a, b, preferred_element_type=F32)

    return dot(left[0], right[0]) + (dot(left[0], right[1]) + dot(left[1], right[0]))


def pair(table, first, last):
    return table[0, :, first:last], table[1, :, first:last]


def stress_kernel(
    occ_any, miller_any, coef_any, dens_any, factor_any, plane_any, column_any,
    totals_out, density_out, square_out,
    occ, millers, coef, dens, far_plane, factor, in_plane, in_column,
    sn, rn, gz, rg, sp, rsp,
    part, twin, qa, qb, ra, rb, ha, hb, a1, b1, ra2, rb2, ab, rz, tmp,
    held, tot_z, tot_p, density, square_held,
    far, lsem, osem, ssem, rsem, bulk_s, bulk_r,
):
    band, s = lax.axis_index("band"), lax.axis_index("spin")
    x_lo, z, y, c = band // 64, lax.rem(band // 8, 8), lax.rem(band // 2, 4), lax.rem(band, 2)
    x = s * 2 + x_lo
    other = 1 - c

    def at(x_=None, z_=None, y_=None, c_=None):
        x_ = x if x_ is None else x_
        z_ = z if z_ is None else z_
        y_ = y if y_ is None else y_
        c_ = c if c_ is None else c_
        return {"band": ((lax.rem(x_, 2) * 8 + z_) * 4 + y_) * 2 + c_, "spin": x_ // 2}

    x_peers = [lax.rem(x + d, 4) for d in (1, 2, 3)]
    y_peers = [lax.rem(y + d, 4) for d in (1, 2, 3)]
    z_peers = [lax.rem(z + d, 8) for d in range(1, 8)]
    plane = [
        at(x_=lax.rem(x + d // 8, 4), y_=lax.rem(y + d // 2, 4), c_=lax.rem(c + d, 2)) for d in range(1, 32)
    ]

    def load(src, dst, k):
        copy = pltpu.make_async_copy(src, dst, lsem.at[k])
        copy.start()
        return copy

    load_occ = load(occ_any, occ, 0)
    load_coef = [
        load(coef_any.at[:, pl.ds(q * 2048, 2048)], coef.at[:, pl.ds(q * 2048, 2048)], 1 + q) for q in range(4)
    ]
    barrier = pltpu.get_barrier_semaphore()
    for p in z_peers:
        pl.semaphore_signal(barrier, inc=1, device_id=at(z_=p), device_id_type=MESH)
    for peer in plane:
        pl.semaphore_signal(barrier, inc=1, device_id=peer, device_id_type=MESH)

    load_dens, load_plane, load_column, load_factor, load_miller = [
        load(src, dst, 5 + k)
        for k, (src, dst) in enumerate(
            ((dens_any, dens), (plane_any, in_plane), (column_any, in_column), (factor_any, factor),
             (miller_any, millers.at[z]))
        )
    ]
    def send(src, dst, k, peer):
        copy = pltpu.make_async_remote_copy(
            src_ref=src, dst_ref=dst, send_sem=ssem.at[0], recv_sem=rsem.at[k], device_id=peer, device_id_type=MESH
        )
        copy.start()
        return copy

    def arrived(ref, sem):
        pltpu.make_async_copy(ref, ref, sem).wait()

    load_occ.wait()
    w0 = jnp.full((64, 128), occ[0, 0].astype(F32)) / occupation_unit
    w1 = jnp.full((64, 128), occ[0, 1].astype(F32)) / occupation_unit

    def squares(i, carry):
        for u in range(2):
            rows = pl.ds(pl.multiple_of(i * 256 + u * 128, 128), 128)
            re = coef[0, rows, :].astype(F32)
            im = coef[1, rows, :].astype(F32)
            tmp[u] = re * re + im * im
            both = w0 * tmp[u, pl.ds(0, 64, stride=2), :] + w1 * tmp[u, pl.ds(1, 64, stride=2), :]
            part[i * 2 + u] = both.reshape(2, 32, 128)
        return carry

    for q in range(4):
        load_coef[q].wait()
        lax.fori_loop(q * 8, q * 8 + 8, squares, 0)

    pl.semaphore_wait(barrier, 38)
    twins = [
        send(part.at[pl.ds(q * 16, 16), other], twin.at[pl.ds(q * 16, 16)], q, at(c_=other)) for q in range(4)
    ]
    load_dens.wait()
    over_spin = send(dens.at[1 - s], far_plane, 4, at(x_=x_peers[1]))
    for p in z_peers:
        pl.semaphore_signal(far, inc=1, device_id=at(z_=p), device_id_type=MESH)

    load_plane.wait()
    sn_flat = sn.reshape(512, 128)
    from_x = product(pair(in_plane, 896, 1024), split(jnp.concatenate([dens[0], dens[1]], axis=1)))
    for zz in range(2):
        sn_flat[pl.ds(zz, 128, stride=4), :] = dens[zz]
        sn_flat[pl.ds(2 + zz, 128, stride=4), :] = from_x[:, zz * 128 : zz * 128 + 128]

    for q in range(4):
        twins[q].wait_recv()

        def add_twin(j, carry):
            for u in range(4):
                i = j * 4 + u
                x_lo_, zz, yy = i // 32, lax.rem(i // 4, 8), u
                v = part[i, c] + twin[i]
                for x_hi in range(2):
                    pos = x_hi * 2 + x_lo_
                    qa[pos, yy * 8 + zz] = v[x_hi * 16 : x_hi * 16 + 8]
                    qb[yy, pos * 8 + zz] = v[x_hi * 16 + 8 : x_hi * 16 + 16]
            return carry

        lax.fori_loop(q * 4, q * 4 + 4, add_twin, 0)
    top, low_half = pl.ds(0, 16), pl.ds(16, 16)
    rings = (
        (qa, ra, ha, x_peers, lambda p: at(x_=p), 6),
        (qb, rb, hb, y_peers, lambda p: at(y_=p), 9),
    )
    for own, got, half, (right, across, left), where, k in rings:
        send(own.at[across, top], half.at[0], k, where(right))
        send(own.at[across, low_half], half.at[1], k, where(left))
    pl.semaphore_wait(far, 7)

    def push_density(t, carry):
        pltpu.make_async_remote_copy(
            src_ref=sn.at[t], dst_ref=rn.at[band], send_sem=bulk_s.at[0], recv_sem=bulk_r.at[0],
            device_id={"band": t}, device_id_type=MESH,
        ).start()
        return carry

    lax.fori_loop(band + 1, 128, push_density, 0)
    lax.fori_loop(0, band, push_density, 0)
    rn[band] = sn[band]

    load_miller.wait()
    for p in z_peers:
        send(millers.at[z], millers.at[z], 5, at(z_=p))

    for own, got, half, (right, across, left), where, k in rings:
        send(own.at[right, low_half], got.at[0, low_half], k + 1, where(right))
        send(own.at[left, top], got.at[1, top], k + 1, where(left))

    over_spin.wait_recv()
    along = product(split(dens[s] + far_plane[...]), pair(in_plane, 0, 512))
    turned = product(pair(in_plane, 640, 896), split(jnp.concatenate([along[:, 0:256], along[:, 256:512]], axis=0)))
    sp_flat = sp.reshape(256, 128)
    for half in range(2):
        sp_flat[half * 128 : half * 128 + 128] = turned[:, half * 128 : half * 128 + 128]

    me = s * 128 + band

    def push_spectrum(to, t, carry):
        pltpu.make_async_remote_copy(
            src_ref=sp.at[to * 128 + t], dst_ref=rsp.at[band * 2 + s], send_sem=bulk_s.at[1], recv_sem=bulk_r.at[1],
            device_id={"band": t, "spin": to}, device_id_type=MESH,
        ).start()
        return carry

    for own, got, half, (right, across, left), where, k in rings:
        arrived(half.at[pl.ds(0, 2)], rsem.at[k])
        half[2] = own[right, top] + half[0]
        send(half.at[2], got.at[0, top], k + 1, where(right))
        half[3] = own[left, low_half] + half[1]
        send(half.at[3], got.at[1, low_half], k + 1, where(left))

    for to, start in ((1 - s, band), (s, band + 1)):
        push = functools.partial(push_spectrum, to)
        lax.fori_loop(start, 128, push, 0)
        lax.fori_loop(0, band, push, 0)
    rsp[band * 2 + s] = sp[me]

    arrived(ra, rsem.at[7])
    for t in range(4):
        sub = pl.ds(t * 8, 8)
        a1[t] = qa[x, sub] + (ra[0, sub] + ra[1, sub])
    for d, p in enumerate(y_peers):
        send(a1.at[p], ra2.at[d], 8, at(y_=p))
    arrived(rb, rsem.at[10])
    for t in range(4):
        sub = pl.ds(t * 8, 8)
        b1[t] = qb[y, sub] + (rb[0, sub] + rb[1, sub])
    for d, p in enumerate(x_peers):
        send(b1.at[p], rb2.at[d], 11, at(x_=p))

    load_column.wait()
    all_n = rn.at[pl.ds(0, 127)]
    arrived(all_n, bulk_r.at[0])
    rn_flat = rn.reshape(512, 128)
    n, grad_x = [
        jnp.concatenate([rn_flat[pl.ds(k, 128, stride=4), :], rn_flat[pl.ds(k + 1, 128, stride=4), :]], axis=0)
        for k in (0, 2)
    ]
    halves_n = split(n)
    grads = (grad_x, product(halves_n, pair(in_plane, 512, 640)), product(pair(in_column, 512, 768), halves_n))
    square = grads[0] * grads[0] + grads[1] * grads[1] + grads[2] * grads[2]
    gz_flat = gz.reshape(256, 128)
    for zz in range(2):
        gz_flat[pl.ds(zz, 128, stride=2), :] = square[zz * 128 : zz * 128 + 128]

    def down(value):
        return jnp.sum(value, axis=0, keepdims=True)

    pairs = ((0, 0), (1, 1), (2, 2), (1, 2), (0, 2), (0, 1))
    room = 4.0 * n * n + 1.0
    kernel = jnp.exp(jnp.log(n) * (-1.0 / 3.0)) * room / (room + square)
    scaled_grads = [kernel * g for g in grads]
    xc = [down(scaled_grads[a] * grads[b]) for a, b in pairs]

    load_factor.wait()
    lane = lax.broadcasted_iota(jnp.int32, (256, 128), 1)
    row = lax.broadcasted_iota(jnp.int32, (256, 128), 0)
    low = lane < 64
    unit_x, unit_y, unit_z = 2.0 * np.pi / NX, 2.0 * np.pi / NY, 2.0 * np.pi / NZ
    ky = jnp.where(low, lane, lane - 64) - 64 * s
    fy = unit_y * ky.astype(F32)
    fz = unit_z * jnp.where(row >= NZ // 2, row - NZ, row).astype(F32)
    fx = unit_x * jnp.full((1, 128), jnp.where(band >= NX // 2, band - NX, band).astype(F32))
    length_sq = fx * fx + fy * fy + fz * fz
    positive = length_sq > 0
    inverse = jnp.where(positive, 1.0 / jnp.where(positive, length_sq, 1.0), 0.0)
    f0, f1 = factor[0], factor[1]
    first = jnp.where(s == 0, f0, pltpu.roll(f0, 64, 1))
    second = jnp.where(s == 0, pltpu.roll(f1, 64, 1), f1)
    local = 2.0 * jnp.where(low, first, second)

    arrived(ra2, rsem.at[8])
    ab[:, 0] = (a1[y] + ra2[0]) + (ra2[1] + ra2[2])
    arrived(rb2, rsem.at[11])
    ab[:, 1] = (b1[x] + rb2[0]) + (rb2[1] + rb2[2])
    for d, p in enumerate(z_peers):
        send(ab.at[p], rz.at[d], 12, at(z_=p))

    arrived(millers.at[pl.ds(0, 7)], rsem.at[5])

    def wave(a, at_z):
        return spacing * (millers[at_z, :, a].astype(F32) + kpoint[a])

    kinetic = [jnp.zeros((1, 128), F32)] * 6
    for at_z in range(8):
        weight = ab[at_z].reshape(16, 128)
        g = [wave(a, at_z) for a in range(3)]
        scaled = [weight * one for one in g]
        kinetic = [t + down(scaled[a] * g[b]) for t, (a, b) in zip(kinetic, pairs)]

    all_sp = rsp.at[pl.ds(0, 255)]
    arrived(all_sp, bulk_r.at[1])
    planes = rsp.reshape(256, 128)[...] * (1.0 / CELLS)
    crossed = pltpu.roll(planes, 64, 1)
    crossed = jnp.where(low, crossed, -crossed)
    spectrum = product(pair(in_column, 0, 512), split(jnp.concatenate([planes, crossed], axis=0)))
    hartree = (4.0 * np.pi) * (spectrum * spectrum) * inverse
    weighting = 2.0 * hartree * inverse + spectrum * local

    sum_h = down(hartree)
    sum_1, sum_z, sum_zz = down(weighting), down(weighting * fz), down(weighting * fz * fz)
    fy1 = fy[0:1]
    spectral = [
        fx * fx * sum_1 - sum_h, fy1 * fy1 * sum_1 - sum_h, sum_zz - sum_h, fy1 * sum_z, fx * sum_z, fx * fy1 * sum_1
    ]

    lines = [spectral[a] - kinetic[a] * (1.0 / NPW) - xc[a] * (1.0 / CELLS) for a in range(6)]
    sums = jnp.sum(jnp.concatenate(lines + [jnp.zeros((2, 128), F32)], axis=0), axis=1, keepdims=True)
    diagonal = lax.broadcasted_iota(jnp.int32, (8, 128), 0) == lax.broadcasted_iota(jnp.int32, (8, 128), 1)
    held[0] = down(jnp.where(diagonal, sums, 0.0))

    def push_back(t, carry):
        pltpu.make_async_remote_copy(
            src_ref=gz.at[t], dst_ref=rg.at[band], send_sem=bulk_s.at[2], recv_sem=bulk_r.at[2],
            device_id={"band": t}, device_id_type=MESH,
        ).start()
        return carry

    plane_me = (x * 4 + y) * 2 + c
    stages = ((tot_z, z, [at(z_=p) for p in z_peers], 8), (tot_p, plane_me, plane, 32))
    for stage, (slots, mine, peers, count) in enumerate(stages):
        for peer in peers:
            pltpu.make_async_remote_copy(
                src_ref=held.at[stage], dst_ref=slots.at[mine], send_sem=ssem.at[1], recv_sem=bulk_r.at[3 + stage],
                device_id=peer, device_id_type=MESH,
            ).start()
        slots[mine] = held[stage]
        if stage == 0:
            lax.fori_loop(band + 1, 128, push_back, 0)
            lax.fori_loop(0, band, push_back, 0)
            rg[band] = gz[band]
        if stage == 1:
            arrived(rz, rsem.at[12])
            weight = ab[z]
            for d in range(7):
                weight = weight + rz[d]
            weight = weight.reshape(16, 128)
            g = [wave(a, z) for a in range(3)]
            density[...] = 0.5 * (g[0] * g[0] + g[1] * g[1] + g[2] * g[2]) * weight
            store_density = pltpu.make_async_copy(density, density_out, osem.at[1])
            store_density.start()
        arrived(slots.at[pl.ds(0, count - 1)], bulk_r.at[3 + stage])
        held[stage + 1] = down(slots.reshape(count, 128)[...])
    store_totals = pltpu.make_async_copy(held.at[2], totals_out, osem.at[2])
    store_totals.start()
    arrived(rg.at[pl.ds(0, 127)], bulk_r.at[2])
    rg_flat = rg.reshape(256, 128)
    for zz in range(2):
        square_held[zz] = rg_flat[pl.ds(zz, 128, stride=2), :]
    store_square = pltpu.make_async_copy(square_held, square_out, osem.at[0])
    store_square.start()

    arrived(coef.at[:, pl.ds(0, 4544)], ssem.at[0])
    arrived(sp.at[pl.ds(0, 38)], ssem.at[1])
    for k, ref in ((0, all_n), (1, all_sp), (2, rg.at[pl.ds(0, 127)])):
        arrived(ref, bulk_s.at[k])
    store_square.wait()
    store_density.wait()
    store_totals.wait()


def emit_kernel(totals_any, density_any, square_any, stress_out, density_out, square_out, totals, stress, density, square, sem):
    into = [
        pltpu.make_async_copy(src, dst, sem.at[k])
        for k, (src, dst) in enumerate(((square_any, square), (density_any, density), (totals_any, totals)))
    ]
    for copy in into:
        copy.start()
    out = [
        pltpu.make_async_copy(src, dst, sem.at[3 + k])
        for k, (src, dst) in enumerate(((square, square_out), (density, density_out), (stress, stress_out)))
    ]
    for k in range(2):
        into[k].wait()
        out[k].start()
    into[2].wait()
    for a in range(6):
        stress[a] = totals[0, a]
    out[2].start()
    for copy in out:
        copy.wait()


def shards(coefficients, occupation, miller, density, local_factor):
    pairs = coefficients[0].reshape(2, 2, NPW // 128, 128).transpose(0, 2, 1, 3).reshape(2, NPW // 64, 128)
    in_plane, in_column = [jnp.asarray(t) for t in tables()]
    hbm = pl.BlockSpec(memory_space=pltpu.HBM)
    millers = miller.reshape(3, 16, 128).transpose(1, 0, 2)
    loaded = [((8, 16, 3, 128), jnp.int32), (pairs.shape, BF16), ((2, 128, 128), F32), ((128, 128), F32), ((2, 256, 128), F32)]
    loaded += [(t.shape, BF16) for t in (in_plane, in_column)]
    scratch = loaded + [
        (shape, F32)
        for shape in (
            (128, 4, 128), (128, 4, 128), (128, 2, 128), (128, 2, 128), (256, 1, 128), (256, 1, 128),
            (64, 2, 32, 128), (64, 32, 128), (4, 32, 8, 128), (4, 32, 8, 128), (2, 32, 8, 128), (2, 32, 8, 128),
            (4, 16, 8, 128), (4, 16, 8, 128),
            (4, 8, 8, 128), (4, 8, 8, 128), (3, 8, 8, 128), (3, 8, 8, 128), (8, 2, 8, 128), (7, 2, 8, 128), (2, 128, 128),
            (3, 1, 128), (8, 1, 128), (32, 1, 128), (16, 128), (2, 128, 128),
        )
    ]
    dma = pltpu.SemaphoreType.DMA
    results = (
        jax.ShapeDtypeStruct((1, 128), F32),
        jax.ShapeDtypeStruct((16, 128), F32),
        jax.ShapeDtypeStruct((2, 128, 128), F32),
    )
    totals, kinetic_density, square = pl.pallas_call(
        stress_kernel,
        out_shape=results,
        in_specs=[hbm] * 7,
        out_specs=(hbm,) * 3,
        scratch_shapes=[pltpu.SMEM((1, 2), jnp.int32)]
        + [pltpu.VMEM(*one) for one in scratch]
        + [pltpu.SemaphoreType.REGULAR, dma((10,)), dma((3,)), dma((2,)), dma((13,)), dma((3,)), dma((5,))],
        compiler_params=pltpu.CompilerParams(collective_id=0, has_side_effects=True),
    )(occupation, millers, pairs, density[0], local_factor.reshape(2, 256, 128), in_plane, in_column)
    stress, kinetic_density, square = pl.pallas_call(
        emit_kernel,
        out_shape=(jax.ShapeDtypeStruct((6,), F32),) + results[1:],
        in_specs=[hbm] * 3,
        out_specs=(hbm,) * 3,
        scratch_shapes=[
            pltpu.SMEM((1, 128), F32),
            pltpu.SMEM((6,), F32),
            pltpu.VMEM((16, 128), F32),
            pltpu.VMEM((2, 128, 128), F32),
            dma((6,)),
        ],
    )(totals, kinetic_density, square)
    return (stress, kinetic_density.reshape(-1), square[None])


def solution(mesh):
    return jax.shard_map(
        shards,
        mesh=mesh,
        in_specs=(
            P("spin", None, "band", None),
            P("spin", "band"),
            P(None, ("band", "spin")),
            P("spin", "band", None, None),
            P(None, None, "band", None),
        ),
        out_specs=(P(), P(("band", "spin")), P("spin", "band", None, None)),
        check_vma=False,
    )
```
